32 devices in a mesh: ctx: 2 (over x), grp: 4 (over y, core), tp: 4 (over z).
Axes of the slice: x: 2, y: 2, z: 4, core: 2. Of those that a mesh axis runs over, the one named last changes fastest.
Arguments:
- tokens: bfloat16 [4096, 4608], P(('grp', 'ctx')), parts along dimension 0, may hold values from -6 to 6
- token_pos: int32 [4096], P(('grp', 'ctx')), parts along dimension 0, may hold values from 0 to 1023, as said below
- norm_gain: float32 [4608], replicated, may hold values from 0.1 to 1.9
- query_weight: bfloat16 [4608, 4096], P('ctx', 'tp'), may hold values from -0.09375 to 0.09375
- key_weight: bfloat16 [4608, 2048], P('ctx', 'tp'), may hold values from -0.09375 to 0.09375
- value_weight: bfloat16 [4608, 2048], P('ctx', 'tp'), may hold values from -0.09375 to 0.09375
Outputs:
- attended: bfloat16 [4096, 4096], P(('grp', 'ctx'), 'tp'), parts along dimension 0
The draws below stay inside these ranges and needn't reach their ends.
There are 4 independent parts, one for each index of `grp`. The reference program is written for one: setup_inputs(seed, part) draws one part's arguments, and reference() takes and returns one part's arrays. A program takes and returns all parts, laid end to end along the dimension named above; an argument that names none is the same for every part. Nothing has to cross between parts.
Inputs may be any that keep to these rules, and one draw needn't show every extreme that they name: `token_pos`: the 512 rows of each index of ctx form two runs of 256 consecutive ascending positions, each starting at a multiple of 256; every position of the sequence occurs exactly once.
All inputs are finite; a program needn't handle non-finite values.
Results may differ from the reference program's by a relative error of at most 0.0077.
Values may be sent and summed in bfloat16 or wider, within the bound.
A program may use at most 128 MiB of HBM per device.

```python
import jax
import jax.numpy as jnp
from jax import lax

D = 4608
HEADS = 32
KV_HEADS = 16
HEAD_DIM = 128
TOK_DEV = 512
TOKENS = 1024


def draw_token_pos(key, part):
    half = TOK_DEV // 2
    devices = TOKENS // TOK_DEV
    blocks = 2 * devices
    order = jax.random.permutation(jax.random.fold_in(key, 12), blocks).astype(jnp.int32)
    target = (jnp.asarray(part).astype(jnp.int32) % blocks).astype(jnp.int32)
    where_target = jnp.argmax((order == target).astype(jnp.int32)).astype(jnp.int32)
    leading = order[0]
    order = order.at[where_target].set(leading)
    order = order.at[0].set(target)
    starts = order * half
    positions = starts[:, None] + jnp.arange(half, dtype=jnp.int32)[None, :]
    return positions.reshape(-1).astype(jnp.int32)


def levels(own_key, shape, shards, smallest, largest):
    def one(axis_at, shards_of):
        steps = jax.random.uniform(jax.random.fold_in(jax.random.fold_in(own_key, 6), axis_at), (shards_of,), jnp.float32, smallest / len(shards), largest / len(shards))
        return jnp.repeat(jnp.exp(steps), shape[axis_at] // shards_of).reshape((-1,) + (1,) * (len(shape) - axis_at - 1))

    factor_of = one(*shards[0])
    for cut in shards[1:]:
        factor_of = factor_of * one(*cut)
    return factor_of


def normal_values(key, shape, spread, reach, split=(), held_as=jnp.bfloat16):
    result = spread * jax.random.normal(key, shape, jnp.float32)
    if split:
        result = result * levels(key, shape, split, -0.22, 0.18)
    return jnp.clip(result, -reach, reach).astype(held_as)


def setup_inputs(seed: int = 0, part: int = 0) -> dict:
    seeds = jax.random.split(jax.random.key(seed), 7)
    own_keys = jax.random.split(jax.random.fold_in(seeds[6], part), 7)
    tokens = normal_values(own_keys[0], (TOKENS, D), 1.0, 6.0, ((0, 2),))
    token_pos = draw_token_pos(jax.random.fold_in(jax.random.fold_in(seeds[6], part), 71), part)
    norm_gain = jnp.clip(1.0 + 0.18 * jax.random.normal(seeds[2], (D,), jnp.float32), 0.1, 1.9)
    query_weight = normal_values(seeds[3], (D, HEADS * HEAD_DIM), D ** -0.5, 0.09375, ((0, 2), (1, 4)))
    key_weight = normal_values(seeds[4], (D, KV_HEADS * HEAD_DIM), D ** -0.5, 0.09375, ((0, 2), (1, 4)))
    value_weight = normal_values(seeds[5], (D, KV_HEADS * HEAD_DIM), D ** -0.5, 0.09375, ((0, 2), (1, 4)))
    return {"tokens": tokens, "token_pos": token_pos, "norm_gain": norm_gain, "query_weight": query_weight, "key_weight": key_weight, "value_weight": value_weight}


query_scale = 144.0 ** (-0.5)

def rotate(field, positions):
    half = field.shape[-1] // 2
    freq = 10000.0 ** (-jnp.arange(half, dtype=jnp.float32) * 2.0 / field.shape[-1])
    angle = positions.astype(jnp.float32)[:, None] * freq[None, :]
    cosine = jnp.cos(angle)[:, None, :]
    sine = jnp.sin(angle)[:, None, :]
    first = field[..., :half]
    second = field[..., half:]
    return jnp.concatenate([first * cosine - second * sine, second * cosine + first * sine], -1)

def reference(tokens, token_pos, norm_gain, query_weight, key_weight, value_weight):
    count = tokens.shape[0]
    inputs = tokens.astype(jnp.float32)
    normed = (inputs * lax.rsqrt(lax.optimization_barrier(jnp.mean(inputs * inputs, -1, keepdims=True)) + 1e-06) * norm_gain[None, :]).astype(jnp.bfloat16)
    queries = jnp.dot(normed, query_weight, preferred_element_type=jnp.float32).reshape(count, HEADS, HEAD_DIM)
    queries = (rotate(queries, token_pos) * query_scale).astype(jnp.bfloat16)
    keys = jnp.dot(normed, key_weight, preferred_element_type=jnp.float32).reshape(count, KV_HEADS, HEAD_DIM)
    keys = rotate(keys, token_pos).astype(jnp.bfloat16)
    values = jnp.dot(normed, value_weight, preferred_element_type=jnp.float32).astype(jnp.bfloat16)
    values = values.reshape(count, KV_HEADS, HEAD_DIM)
    key_full = lax.optimization_barrier(keys).astype(jnp.float32)
    value_full = lax.optimization_barrier(values).astype(jnp.float32)
    half = TOK_DEV // 2
    query_blocks = queries.reshape(count // half, half, KV_HEADS, 2, HEAD_DIM)
    pos_blocks = token_pos.reshape(count // half, half)

    def block(args):
        query_part, pos_part = args
        query_part = lax.optimization_barrier(query_part).astype(jnp.float32)
        scores = jnp.einsum('ngrd,mgd->grnm', query_part, key_full)
        capped = 50.0 * jnp.tanh(scores / 50.0)
        allowed = token_pos[None, None, None, :] <= pos_part[None, None, :, None]
        weights = jnp.where(allowed, jnp.exp(capped), 0.0).astype(jnp.bfloat16)
        weights = lax.optimization_barrier(weights).astype(jnp.float32)
        numerator = jnp.einsum('grnm,mgd->ngrd', weights, value_full)
        total = lax.optimization_barrier(jnp.sum(weights, -1))
        return (numerator / jnp.transpose(total, (2, 0, 1))[..., None]).astype(jnp.bfloat16)
    attended = lax.map(block, (query_blocks, pos_blocks))
    return attended.reshape(count, HEADS * HEAD_DIM)
```

```python
import functools
import math

import jax
import jax.numpy as jnp
import numpy as np
from jax import lax
from jax.experimental import pallas as pl
from jax.experimental.pallas import tpu as pltpu
from jax.sharding import PartitionSpec as P

HEAD_DIM = 128
BLOCK = 2 * HEAD_DIM
MESH = pl.DeviceIdType.MESH

query_scale = 144.0 ** (-0.5)


def each(start, stop, body):
    if stop - start == 1:
        body(start)
    elif stop > start:
        lax.fori_loop(start, stop, lambda i, _: (body(i), None)[1], None)


def kernel(
    n, grp, pos_ref, freq_ref, gain_ref, tok_ref, q_ref, k_ref, v_ref, out_ref,
    wbuf, normed, kvbuf, posbuf, qbuf, acc, cos_ref, sin_ref, qpos_ref,
    tok_sem, own_sem, x_send, x_recv, y_send, y_recv, s_send, s_recv, t_send, t_recv,
    kv_send, kv_recv, pos_send, pos_recv,
):
    c = lax.axis_index("ctx")
    g = lax.axis_index("grp")
    pairs = grp // 2
    near = g % 2
    pair = g // 2
    sibling = pair * 2 + (1 - near)
    depth = q_ref.shape[0]
    part = depth // grp
    rows = tok_ref.shape[0]
    kv_blocks = k_ref.shape[1] // BLOCK
    groups = k_ref.shape[1] // HEAD_DIM
    q_blocks = q_ref.shape[1] // BLOCK
    sources = [(k_ref, i) for i in range(kv_blocks)]
    sources += [(v_ref, i) for i in range(kv_blocks)]
    sources += [(q_ref, i) for i in range(q_blocks)]
    blocks = len(sources)

    def region(owner, member):
        return pl.ds(pl.multiple_of(owner * depth + member * part, 16), part)

    def peer(d):
        return lax.rem(c + d, n)

    def source(d):
        return lax.rem(c + n - d, n)

    def far(j):
        return lax.rem(pair + j, pairs)

    def near_of(j):
        return lax.rem(pair + pairs - j, pairs)

    def x_copy(b, d):
        return pltpu.make_async_remote_copy(
            src_ref=wbuf.at[b, region(c, g)], dst_ref=wbuf.at[b, region(c, g)],
            send_sem=x_send.at[b, d - 1], recv_sem=x_recv.at[b, d - 1],
            device_id={"ctx": peer(d)}, device_id_type=MESH,
        )

    def hop(b, where, send, recv, member):
        return pltpu.make_async_remote_copy(
            src_ref=wbuf.at[b, where], dst_ref=wbuf.at[b, where],
            send_sem=send, recv_sem=recv, device_id={"grp": member}, device_id_type=MESH,
        )

    def y_copy(b, d, j):
        return hop(b, region(source(d), g), y_send.at[b, d - 1, j - 1], y_recv.at[b, d - 1, j - 1],
                   far(j) * 2 + near)

    def y_wait(b, d, j):
        hop(b, region(source(d), near_of(j) * 2 + near), y_send.at[b, d - 1, j - 1],
            y_recv.at[b, d - 1, j - 1], sibling).wait_recv()

    def s_copy(b, d):
        return hop(b, region(source(d), g), s_send.at[b, d - 1], s_recv.at[b, d - 1], sibling)

    def s_wait(b, d):
        hop(b, region(source(d), sibling), s_send.at[b, d - 1], s_recv.at[b, d - 1],
            sibling).wait_recv()

    def t_copy(b, d, j):
        return hop(b, region(source(d), near_of(j) * 2 + near), t_send.at[b, d - 1, j - 1],
                   t_recv.at[b, d - 1, j - 1], sibling)

    def t_wait(b, d, j):
        hop(b, region(source(d), near_of(j) * 2 + 1 - near), t_send.at[b, d - 1, j - 1],
            t_recv.at[b, d - 1, j - 1], sibling).wait_recv()

    def kv_copy(b, d, owner):
        return pltpu.make_async_remote_copy(
            src_ref=kvbuf.at[b, owner], dst_ref=kvbuf.at[b, owner],
            send_sem=kv_send.at[b, d - 1], recv_sem=kv_recv.at[b, d - 1],
            device_id={"ctx": peer(d)}, device_id_type=MESH,
        )

    def pos_copy(d, owner):
        return pltpu.make_async_remote_copy(
            src_ref=posbuf.at[owner], dst_ref=posbuf.at[owner],
            send_sem=pos_send.at[d - 1], recv_sem=pos_recv.at[d - 1],
            device_id={"ctx": peer(d)}, device_id_type=MESH,
        )

    def own_copy(b):
        ref, col = sources[b]
        return pltpu.make_async_copy(
            ref.at[:, pl.ds(col * BLOCK, BLOCK)],
            wbuf.at[b, pl.ds(pl.multiple_of(c * depth, 16), depth)], own_sem.at[b],
        )

    tok_copy = pltpu.make_async_copy(tok_ref, normed, tok_sem)
    own_copy(0).start()
    own_copy(1).start()
    tok_copy.start()
    for b in range(2, blocks):
        own_copy(b).start()

    barrier = pltpu.get_barrier_semaphore()

    def greet(**where):
        pl.semaphore_signal(barrier, inc=1, device_id=where, device_id_type=MESH)

    each(1, n, lambda d: greet(ctx=peer(d)))
    each(1, pairs, lambda j: greet(grp=far(j) * 2 + near))
    greet(grp=sibling)
    pl.semaphore_wait(barrier, n - 1 + pairs - 1 + 1)

    def send_block(b):
        own_copy(b).wait()
        each(1, n, lambda d: x_copy(b, d).start())

    send_block(0)
    send_block(1)

    lanes = pos_ref[...][None, :]
    posbuf[c] = jnp.broadcast_to(lanes, posbuf.shape[1:])
    qpos = jnp.transpose(
        jnp.broadcast_to(lanes.astype(jnp.float32), (HEAD_DIM, rows)), (1, 0)
    )
    qpos_ref[...] = qpos
    angle = qpos * freq_ref[...]
    lane = lax.broadcasted_iota(jnp.int32, angle.shape, 1)
    sine = jnp.sin(angle)
    cos_ref[...] = jnp.cos(angle)
    sin_ref[...] = jnp.where(lane < HEAD_DIM // 2, -sine, sine)

    tok_copy.wait()
    strip = 32

    def norm_rows(i):
        where = pl.ds(pl.multiple_of(i * strip, strip), strip)
        inputs = normed[where, :].astype(jnp.float32)
        mean = jnp.mean(inputs * inputs, -1, keepdims=True)
        normed[where, :] = (inputs * lax.rsqrt(mean + 1e-06) * gain_ref[...][None, :]).astype(jnp.bfloat16)

    each(0, rows // strip, norm_rows)

    tall = math.gcd(rows, 256)

    def project(b, store, rope, scale):
        def tile(i):
            where = pl.ds(pl.multiple_of(i * tall, tall), tall)
            field = jnp.dot(normed[where, :], wbuf[b], preferred_element_type=jnp.float32)
            if rope:
                cosine, sine = cos_ref[where, :], sin_ref[where, :]
                halves = []
                for h in range(2):
                    one = field[:, h * HEAD_DIM : (h + 1) * HEAD_DIM]
                    halves.append(one * cosine + pltpu.roll(one, HEAD_DIM // 2, 1) * sine)
                field = jnp.concatenate(halves, -1)
            if scale is not None:
                field = field * scale
            store(where, field.astype(jnp.bfloat16))

        each(0, rows // tall, tile)

    def attend(b, owner, first, last):
        def tile(i):
            where = pl.ds(pl.multiple_of(i * tall, tall), tall)
            keys = kvbuf[b, owner]
            values = kvbuf[groups + b, owner]
            values = jnp.concatenate([values, jnp.ones_like(values)], -1)
            key_pos = posbuf[owner, 0:1, :].astype(jnp.float32)
            allowed = key_pos <= qpos_ref[where, 0:1]
            for h in range(2):
                cols = pl.ds(h * HEAD_DIM, HEAD_DIM)
                scores = lax.dot_general(
                    qbuf[b, where, cols], keys, (((1,), (1,)), ((), ())),
                    preferred_element_type=jnp.float32,
                )
                capped = jnp.tanh(scores * (1.0 / 50.0)) * (50.0 * math.log2(math.e))
                weights = jnp.where(allowed, jnp.exp2(capped), 0.0).astype(jnp.bfloat16)
                both = jnp.dot(weights, values, preferred_element_type=jnp.float32)
                if not first:
                    both = both + acc[b, h, where, :]
                if last:
                    done = both[:, :HEAD_DIM] / both[:, HEAD_DIM:]
                    out_ref[where, pl.ds(b * BLOCK + h * HEAD_DIM, HEAD_DIM)] = done.astype(
                        out_ref.dtype
                    )
                else:
                    acc[b, h, where, :] = both

        each(0, rows // tall, tile)

    received = set()

    def attend_others(b):
        if "pos" not in received:
            received.add("pos")
            each(1, n, lambda d: pos_copy(d, source(d)).wait_recv())
        for index in (b, groups + b):
            if index not in received:
                received.add(index)
                each(1, n, lambda d: kv_copy(index, d, source(d)).wait_recv())
        each(1, n - 1, lambda d: attend(b, source(d), False, False))
        attend(b, source(n - 1), False, True)

    def send_group(h):
        each(1, n, lambda d: kv_copy(h, d, c).start())
        each(1, n, lambda d: kv_copy(groups + h, d, c).start())

    def store_kv(first):
        def store(where, field):
            kvbuf[first, c, where, :] = field[:, :HEAD_DIM]
            kvbuf[first + 1, c, where, :] = field[:, HEAD_DIM:]

        return store

    def store_q(h):
        def store(where, field):
            qbuf[h, where, :] = field

        return store

    for t in range(blocks + 2):
        if t < blocks:
            def forward(d, b=t):
                x_copy(b, d).wait_recv()
                each(1, pairs, lambda j: y_copy(b, d, j).start())
                s_copy(b, d).start()

            each(1, n, forward)
        if 1 <= t <= blocks:
            def onward(d, b=t - 1):
                def one(j):
                    y_wait(b, d, j)
                    t_copy(b, d, j).start()

                each(1, pairs, one)

            each(1, n, onward)
        if t >= 2:
            b = t - 2

            def arrive(d, b=b):
                s_wait(b, d)
                each(1, pairs, lambda j: t_wait(b, d, j))

            each(1, n, arrive)
            if b < 2 * kv_blocks:
                project(b, store_kv(2 * b), b < kv_blocks, None)
        if t + 2 < blocks:
            send_block(t + 2)
        if t == 2:
            each(1, n, lambda d: pos_copy(d, c).start())
        if t >= blocks - 2:
            share = [h for h in range(groups) if min(blocks - 2 + h, blocks) == t]
            for h in share:
                send_group(h)
        if t >= 2 and t - 2 >= 2 * kv_blocks:
            h = t - 2 - 2 * kv_blocks
            project(t - 2, store_q(h), True, query_scale)
            attend(h, c, True, False)
            if t == blocks:
                attend_others(0)
    for h in range(1, q_blocks):
        attend_others(h)

    def settle(d):
        pos_copy(d, c).wait_send()
        for b in range(2 * groups):
            kv_copy(b, d, c).wait_send()
        for b in range(blocks):
            x_copy(b, d).wait_send()
            s_copy(b, d).wait_send()

            def pair_sends(j, b=b):
                y_copy(b, d, j).wait_send()
                t_copy(b, d, j).wait_send()

            each(1, pairs, pair_sends)

    each(1, n, settle)


def write_out(in_ref, out_ref, sem):
    copy = pltpu.make_async_copy(in_ref, out_ref, sem)
    copy.start()
    copy.wait()


def on_device(n, grp, tokens, token_pos, norm_gain, query_weight, key_weight, value_weight):
    rows, width = tokens.shape
    depth, q_cols = query_weight.shape
    kv_cols = key_weight.shape[1]
    q_blocks, kv_blocks = q_cols // BLOCK, kv_cols // BLOCK
    blocks = q_blocks + 2 * kv_blocks
    pairs = grp // 2
    half = HEAD_DIM // 2
    freq = 10000.0 ** (-np.arange(half) * 2.0 / HEAD_DIM)
    freq = np.concatenate([freq, freq])[None, :].astype(np.float32)
    dma = pltpu.SemaphoreType.DMA
    far = max(pairs - 1, 1)
    vmem = pl.BlockSpec(memory_space=pltpu.VMEM)
    anywhere = pl.BlockSpec(memory_space=pl.ANY)
    held = [pltpu.with_memory_space_constraint(x, pltpu.HBM) for x in (tokens, query_weight, key_weight, value_weight)]
    attended = pl.pallas_call(
        functools.partial(kernel, n, grp),
        out_shape=pltpu.VMEM((rows, q_cols), jnp.bfloat16),
        in_specs=[vmem] * 3 + [pl.BlockSpec(memory_space=pltpu.HBM)] * 4,
        out_specs=vmem,
        scratch_shapes=[
            pltpu.VMEM((blocks, n * depth, BLOCK), jnp.bfloat16),
            pltpu.VMEM((rows, width), jnp.bfloat16),
            pltpu.VMEM((4 * kv_blocks, n, rows, HEAD_DIM), jnp.bfloat16),
            pltpu.VMEM((n, 8, rows), jnp.int32),
            pltpu.VMEM((q_blocks, rows, BLOCK), jnp.bfloat16),
            pltpu.VMEM((q_blocks, 2, rows, BLOCK), jnp.float32),
            pltpu.VMEM((rows, HEAD_DIM), jnp.float32),
            pltpu.VMEM((rows, HEAD_DIM), jnp.float32),
            pltpu.VMEM((rows, HEAD_DIM), jnp.float32),
            dma(()),
            dma((blocks,)),
            dma((blocks, n - 1)),
            dma((blocks, n - 1)),
            dma((blocks, n - 1, far)),
            dma((blocks, n - 1, far)),
            dma((blocks, n - 1)),
            dma((blocks, n - 1)),
            dma((blocks, n - 1, far)),
            dma((blocks, n - 1, far)),
            dma((4 * kv_blocks, n - 1)),
            dma((4 * kv_blocks, n - 1)),
            dma((n - 1,)),
            dma((n - 1,)),
        ],
        compiler_params=pltpu.CompilerParams(
            collective_id=0, has_side_effects=True, vmem_limit_bytes=44 * 1024 * 1024
        ),
    )(token_pos, freq, norm_gain, *held)
    return pl.pallas_call(
        write_out,
        out_shape=jax.ShapeDtypeStruct(attended.shape, attended.dtype),
        in_specs=[vmem],
        out_specs=anywhere,
        scratch_shapes=[dma(())],
        compiler_params=pltpu.CompilerParams(vmem_limit_bytes=4 * 1024 * 1024),
    )(attended)


def pair_kernel(
    line, pos_ref, freq_ref, gain_ref, tok_ref, q_ref, k_ref, v_ref, out_ref,
    xbuf, oth, near, wbuf, psend, precv, acc, kbuf, vbuf, qbuf, obuf, cos_ref, sin_ref, qpos_ref,
    factor_ref, kpos_ref, side, pos_in, freq_in, gain_in, gain_row,
    tok_sem, w_sem, in_sem, side_send, side_recv, x_send, x_recv, up_send, up_recv, dn_send, dn_recv,
    p_send, p_recv, r_send, r_recv, o_send, o_recv,
):
    c = lax.axis_index("ctx")
    z = lax.axis_index("tp")
    o = 1 - c
    rows, half = oth.shape
    heads = wbuf.shape[0]
    mine = heads // 2
    quarter = rows // line
    subs = x_send.shape[0]
    strip = quarter // subs
    tall = math.gcd(rows, 256)
    tiles = rows // tall
    last = line - 1

    def at_least(k):
        return (z + line - k) // line

    order = [sorted(range(line), key=lambda q, k=k: (abs(q - k), q)) for k in range(line)]

    def stage_quarter(s):
        q = order[0][s]
        for k in range(1, line):
            q = q + (order[k][s] - order[k - 1][s]) * at_least(k)
        return q

    def band(q, i=0, size=quarter):
        return pl.ds(pl.multiple_of(q * quarter + i * size, strip), size)

    def columns(side, i, width):
        return pl.ds(pl.multiple_of((side * mine + i) * width, HEAD_DIM), width)

    def features(side):
        return pl.ds(pl.multiple_of(side * half, HEAD_DIM), half)

    def w_copies(s):
        side, i = (o, s) if s < mine else (c, s - mine)
        parts = [
            (k_ref, HEAD_DIM, 0), (v_ref, HEAD_DIM, HEAD_DIM), (q_ref, BLOCK, 2 * HEAD_DIM),
        ]
        return [
            pltpu.make_async_copy(
                ref.at[:, columns(side, i, width)], wbuf.at[s, :, pl.ds(at, width)], w_sem.at[s, p]
            )
            for p, (ref, width, at) in enumerate(parts)
        ]

    def tok_copies(j):
        where = band(lax.rem(z + j, line))
        return [
            pltpu.make_async_copy(tok_ref.at[where, features(c)], xbuf.at[0, where], tok_sem.at[j, 0]),
            pltpu.make_async_copy(tok_ref.at[where, features(o)], oth.at[where], tok_sem.at[j, 1]),
        ]

    def start(copies):
        for copy in copies:
            copy.start()

    def wait(copies):
        for copy in copies:
            copy.wait()

    def remote(src, dst, send, recv, **where):
        return pltpu.make_async_remote_copy(
            src_ref=src, dst_ref=dst, send_sem=send, recv_sem=recv,
            device_id=where, device_id_type=MESH,
        )

    def x_copy(i):
        where = band(z, i, strip)
        return remote(oth.at[where], xbuf.at[1, where], x_send.at[i], x_recv.at[i], ctx=o)

    def up_copy(e, hops):
        where = band(z - hops - e // subs, e % subs, strip)
        return remote(xbuf.at[1, where], xbuf.at[1, where], up_send.at[e], up_recv.at[e], tp=z + 1 - 2 * hops)

    def dn_copy(e, hops):
        where = band(z + hops + e // subs, e % subs, strip)
        return remote(xbuf.at[1, where], xbuf.at[1, where], dn_send.at[e], dn_recv.at[e], tp=z - 1 + 2 * hops)

    def side_copy():
        return remote(side.at[0], side.at[1], side_send, side_recv, ctx=o)

    def p_copy(i, t):
        where = pl.ds(t * tall, tall)
        return remote(psend.at[0, i, where], precv.at[1, i, where], p_send.at[i, t], p_recv.at[i, t], ctx=o)

    def r_copy(i, s):
        where = band(stage_quarter(s))
        return remote(psend.at[1, i, where], precv.at[0, i, where], r_send.at[i, s], r_recv.at[i, s], ctx=o)

    def o_copy(i, t, side):
        where = pl.ds(t * tall, tall)
        return remote(
            obuf.at[i, where], out_ref.at[side * mine + i, where], o_send.at[i, t], o_recv.at[i, t], ctx=o
        )

    small = [
        pltpu.make_async_copy(gain_ref, gain_in, in_sem.at[0]),
        pltpu.make_async_copy(pos_ref, pos_in, in_sem.at[1]),
        pltpu.make_async_copy(freq_ref, freq_in, in_sem.at[2]),
    ]
    ahead = tok_copies(0)
    ahead[1].start()
    start(small)

    barrier = pltpu.get_barrier_semaphore()

    def greet(**where):
        pl.semaphore_signal(barrier, inc=1, device_id=where, device_id_type=MESH)

    greet(ctx=o)

    @pl.when(z > 0)
    def _():
        greet(tp=z - 1)

    @pl.when(z < last)
    def _():
        greet(tp=z + 1)

    ahead[0].start()
    for j in range(1, line):
        start(tok_copies(j))
    ahead[1].wait()
    pl.semaphore_wait(barrier, 1 + at_least(1) + 1 - at_least(last))
    for i in range(subs):
        x_copy(i).start()
    for s in range(heads):
        start(w_copies(s))

    vbuf[...] = jnp.ones_like(vbuf)
    wait(small)
    gain_row[...] = gain_in[...][None, :]
    side[0, 0:8, :] = jnp.broadcast_to(pos_in[...][None, :], (8, rows)).astype(jnp.float32)

    def norm_rows(where):
        own = xbuf[0, where, :].astype(jnp.float32)
        other = oth[where, :].astype(jnp.float32)
        total = jnp.sum(own * own, -1, keepdims=True) + jnp.sum(other * other, -1, keepdims=True)
        factor = lax.rsqrt(total * (1.0 / (2 * half)) + 1e-06)
        factor_ref[where, :] = jnp.broadcast_to(factor, (strip, HEAD_DIM))
        xbuf[0, where, :] = (own * factor * gain_row[:, features(c)]).astype(jnp.bfloat16)

    def norm_quarter(j):
        wait(ahead[:1] if j == 0 else tok_copies(j))
        each(0, subs, lambda i: norm_rows(band(lax.rem(z + j, line), i, strip)))

    def norm_far(q):
        def one(i):
            where = band(q, i, strip)
            raw = xbuf[1, where, :].astype(jnp.float32)
            normed = raw * factor_ref[where, 0:1] * gain_row[:, features(c)]
            near[pl.ds(pl.multiple_of(i * strip, strip), strip), :] = normed.astype(jnp.bfloat16)

        each(0, subs, one)

    def product(rows_in, s):
        return jnp.dot(rows_in, wbuf[s], preferred_element_type=jnp.float32)

    def tile(t):
        return pl.ds(pl.multiple_of(t * tall, tall), tall)

    loaded = set()

    def load(s):
        if s not in loaded:
            loaded.add(s)
            wait(w_copies(s))

    def own_product(i):
        load(i)

        def one(t):
            psend[0, i, tile(t), :] = product(xbuf[0, tile(t), :], i).astype(jnp.bfloat16)

        each(0, tiles, one)
        for t in range(tiles):
            p_copy(i, t).start()

    def own_local(i):
        load(mine + i)

        def one(t):
            acc[0, i, tile(t), :] = product(xbuf[0, tile(t), :], mine + i)

        each(0, tiles, one)

    def far_product(i, s):
        load(i)
        where = band(stage_quarter(s))
        psend[1, i, where, :] = product(near[...], i).astype(jnp.bfloat16)

    def far_local(i, s):
        load(mine + i)
        where = band(stage_quarter(s))
        acc[1, i, where, :] = product(near[...], mine + i)

    def angles(slot):
        where = pl.ds(slot * rows, rows)
        lanes = side[slot, 0:1, :]
        kpos_ref[:, where] = jnp.broadcast_to(lanes, (8, rows))
        qpos = jnp.transpose(jnp.broadcast_to(lanes, (HEAD_DIM, rows)), (1, 0))
        qpos_ref[where, :] = qpos
        angle = qpos * freq_in[...]
        lane = lax.broadcasted_iota(jnp.int32, angle.shape, 1)
        sine = jnp.sin(angle)
        cos_ref[where, :] = jnp.cos(angle)
        sin_ref[where, :] = jnp.where(lane < HEAD_DIM // 2, -sine, sine)

    def finish(i, slot):
        def one(t):
            where = tile(t)
            at = pl.ds(pl.multiple_of(slot * rows + t * tall, tall), tall)
            field = acc[slot, i, where, :] + precv[slot, i, where, :].astype(jnp.float32)
            cosine, sine = cos_ref[at, :], sin_ref[at, :]

            def rope(x):
                return x * cosine + pltpu.roll(x, HEAD_DIM // 2, 1) * sine

            kbuf[i, at, :] = rope(field[:, :HEAD_DIM]).astype(jnp.bfloat16)
            vbuf[i, at, :HEAD_DIM] = field[:, HEAD_DIM : 2 * HEAD_DIM].astype(jnp.bfloat16)
            for h in range(2):
                one = field[:, (2 + h) * HEAD_DIM : (3 + h) * HEAD_DIM]
                qbuf[i, at, h * HEAD_DIM : (h + 1) * HEAD_DIM] = (rope(one) * query_scale).astype(jnp.bfloat16)

        each(0, tiles, one)

    def attend(i, slot, t, store):
        at = pl.ds(pl.multiple_of(slot * rows + t * tall, tall), tall)
        for h in range(2):
            both = None
            for part in range(2):
                span = pl.ds(part * rows, rows)
                scores = lax.dot_general(
                    qbuf[i, at, h * HEAD_DIM : (h + 1) * HEAD_DIM], kbuf[i, span, :],
                    (((1,), (1,)), ((), ())), preferred_element_type=jnp.float32,
                )
                allowed = kpos_ref[0:1, span] <= qpos_ref[at, 0:1]
                capped = jnp.tanh(scores * (1.0 / 50.0)) * (50.0 * math.log2(math.e))
                weights = jnp.where(allowed, jnp.exp2(capped), 0.0).astype(jnp.bfloat16)
                more = jnp.dot(weights, vbuf[i, span, :], preferred_element_type=jnp.float32)
                both = more if both is None else both + more
            done = (both[:, :HEAD_DIM] / both[:, HEAD_DIM:]).astype(jnp.bfloat16)
            store(h, done)

    def attend_far(i):
        for t in range(tiles):
            def store(h, done, t=t):
                obuf[i, t * tall : (t + 1) * tall, h * HEAD_DIM : (h + 1) * HEAD_DIM] = done

            attend(i, 1, t, store)
            o_copy(i, t, c).start()

    def attend_own(i):
        def one(t):
            def store(h, done):
                out_ref[c * mine + i, tile(t), h * HEAD_DIM : (h + 1) * HEAD_DIM] = done

            attend(i, 0, t, store)

        each(0, tiles, one)

    def pass_on(r):
        if r < subs:
            x_copy(r).wait_recv()

            @pl.when(z < last)
            def _():
                up_copy(r, 0).start()

            @pl.when(z > 0)
            def _():
                dn_copy(r, 0).start()

        e = r - 1
        if 0 <= e < last * subs:
            @pl.when(z >= 1 + e // subs)
            def _():
                up_copy(e, 1).wait_recv()
                if e + subs < last * subs:
                    @pl.when(z < last)
                    def _():
                        up_copy(e + subs, 0).start()

            @pl.when(z + 1 + e // subs <= last)
            def _():
                dn_copy(e, 1).wait_recv()
                if e + subs < last * subs:
                    @pl.when(z > 0)
                    def _():
                        dn_copy(e + subs, 0).start()

    def stage(s):
        norm_far(stage_quarter(s))
        far_product(0, s)
        r_copy(0, s).start()
        for i in range(1, mine):
            far_product(i, s)
            early = line - 2
            for done in range(early) if s == last - 1 else range(early, line) if s == last else ():
                r_copy(i, done).start()
        for i in range(mine):
            far_local(i, s)

    def far_side():
        side_copy().wait_recv()
        lanes = jnp.broadcast_to(side[1, 8:9, :], (HEAD_DIM, rows))
        factor_ref[...] = jnp.transpose(lanes, (1, 0))

    rounds = 1 + last * subs
    work = {r: [] for r in range(rounds)}
    stage_at = [subs - 1] + [s * subs for s in range(1, line)]
    for s in range(line - 1):
        work[stage_at[s]].append(functools.partial(stage, s))
    work[stage_at[0]].insert(0, far_side)
    fill = [functools.partial(own_product, i) for i in range(mine)]
    fill += [functools.partial(angles, 0)]
    fill += [functools.partial(own_local, i) for i in range(mine)]
    fill += [functools.partial(angles, 1)]

    for j in range(line):
        norm_quarter(j)
    side[0, 8:16, :] = jnp.transpose(factor_ref[...], (1, 0))[0:8, :]
    side_copy().start()
    for r in range(rounds):
        pass_on(r)
        if work[r]:
            for task in work[r]:
                task()
        elif fill:
            fill.pop(0)()
    for task in fill:
        task()

    stage(last)
    for i in range(mine):
        for t in range(tiles):
            p_copy(i, t).wait_recv()
        finish(i, 1)
    for i in range(mine):
        for s in range(line):
            r_copy(i, s).wait_recv()
        finish(i, 0)
        attend_far(i)
        attend_own(i)
    for i in range(mine):
        for t in range(tiles):
            o_copy(i, t, o).wait_recv()

    side_copy().wait_send()
    for i in range(subs):
        x_copy(i).wait_send()
    for e in range(last * subs):
        @pl.when((z < last) & (z >= e // subs))
        def _():
            up_copy(e, 0).wait_send()

        @pl.when((z > 0) & (z + e // subs <= last))
        def _():
            dn_copy(e, 0).wait_send()

    for i in range(mine):
        for t in range(tiles):
            p_copy(i, t).wait_send()
            o_copy(i, t, c).wait_send()
        for s in range(line):
            r_copy(i, s).wait_send()


def write_heads(in_ref, out_ref, sem):
    heads, _, width = in_ref.shape
    copies = [
        pltpu.make_async_copy(in_ref.at[h], out_ref.at[:, pl.ds(h * width, width)], sem.at[h])
        for h in range(heads)
    ]
    for copy in copies:
        copy.start()
    for copy in copies:
        copy.wait()


def rope_freq():
    half = HEAD_DIM // 2
    freq = 10000.0 ** (-np.arange(half) * 2.0 / HEAD_DIM)
    return np.concatenate([freq, freq])[None, :].astype(np.float32)


def on_pair(line, tokens, token_pos, norm_gain, query_weight, key_weight, value_weight):
    rows, width = tokens.shape
    depth, q_cols = query_weight.shape
    heads = key_weight.shape[1] // HEAD_DIM
    mine = heads // 2
    tiles = rows // math.gcd(rows, 256)
    subs = max(rows // line // 32, 1)
    dma = pltpu.SemaphoreType.DMA
    vmem = pl.BlockSpec(memory_space=pltpu.VMEM)
    anywhere = pl.BlockSpec(memory_space=pl.ANY)
    hbm = pl.BlockSpec(memory_space=pltpu.HBM)
    ins = (token_pos, jnp.asarray(rope_freq()), norm_gain, tokens, query_weight, key_weight, value_weight)
    held = [pltpu.with_memory_space_constraint(x, pltpu.HBM) for x in ins]
    bf16, f32 = jnp.bfloat16, jnp.float32
    along = max((line - 1) * subs, 1)
    attended = pl.pallas_call(
        functools.partial(pair_kernel, line),
        out_shape=pltpu.VMEM((heads, rows, BLOCK), bf16),
        in_specs=[hbm] * 7,
        out_specs=vmem,
        scratch_shapes=[
            pltpu.VMEM((2, rows, depth), bf16),
            pltpu.VMEM((rows, depth), bf16),
            pltpu.VMEM((rows // line, depth), bf16),
            pltpu.VMEM((heads, depth, 2 * BLOCK), bf16),
            pltpu.VMEM((2, mine, rows, 2 * BLOCK), bf16),
            pltpu.VMEM((2, mine, rows, 2 * BLOCK), bf16),
            pltpu.VMEM((2, mine, rows, 2 * BLOCK), f32),
            pltpu.VMEM((mine, 2 * rows, HEAD_DIM), bf16),
            pltpu.VMEM((mine, 2 * rows, BLOCK), bf16),
            pltpu.VMEM((mine, 2 * rows, BLOCK), bf16),
            pltpu.VMEM((mine, rows, BLOCK), bf16),
            pltpu.VMEM((2 * rows, HEAD_DIM), f32),
            pltpu.VMEM((2 * rows, HEAD_DIM), f32),
            pltpu.VMEM((2 * rows, HEAD_DIM), f32),
            pltpu.VMEM((rows, HEAD_DIM), f32),
            pltpu.VMEM((8, 2 * rows), f32),
            pltpu.VMEM((2, 16, rows), f32),
            pltpu.VMEM((rows,), jnp.int32),
            pltpu.VMEM((1, HEAD_DIM), f32),
            pltpu.VMEM((width,), f32),
            pltpu.VMEM((1, width), f32),
            dma((line, 2)),
            dma((heads, 3)),
            dma((3,)),
            dma(()),
            dma(()),
            dma((subs,)),
            dma((subs,)),
            dma((along,)),
            dma((along,)),
            dma((along,)),
            dma((along,)),
            dma((mine, tiles)),
            dma((mine, tiles)),
            dma((mine, line)),
            dma((mine, line)),
            dma((mine, tiles)),
            dma((mine, tiles)),
        ],
        compiler_params=pltpu.CompilerParams(
            collective_id=0, has_side_effects=True, vmem_limit_bytes=44 * 1024 * 1024
        ),
    )(*held)
    return pl.pallas_call(
        write_heads,
        out_shape=jax.ShapeDtypeStruct((rows, q_cols), bf16),
        in_specs=[vmem],
        out_specs=anywhere,
        scratch_shapes=[dma((heads,))],
        compiler_params=pltpu.CompilerParams(vmem_limit_bytes=4 * 1024 * 1024),
    )(attended)


def solution(mesh):
    in_specs = (
        P(("grp", "ctx"), None),
        P(("grp", "ctx")),
        P(),
        P("ctx", "tp"),
        P("ctx", "tp"),
        P("ctx", "tp"),
    )
    out_specs = P(("grp", "ctx"), "tp")
    ctx, grp, line = (mesh.shape[name] for name in ("ctx", "grp", "tp"))

    def local(tokens, token_pos, norm_gain, query_weight, key_weight, value_weight):
        rows, width = tokens.shape
        depth, kv_cols = key_weight.shape
        heads = kv_cols // HEAD_DIM
        paired = ctx == 2 and width == 2 * depth and heads % 2 == 0
        paired = paired and line > 1 and rows % (line * 32) == 0
        plan = functools.partial(on_pair, line) if paired else functools.partial(on_device, ctx, grp)
        return plan(tokens, token_pos, norm_gain, query_weight, key_weight, value_weight)

    return jax.shard_map(
        local, mesh=mesh, in_specs=in_specs, out_specs=out_specs, check_vma=False,
    )
```

```python
import functools
import math

import jax
import jax.numpy as jnp
import numpy as np
from jax import lax
from jax.experimental import pallas as pl
from jax.experimental.pallas import tpu as pltpu
from jax.sharding import PartitionSpec as P

HEAD_DIM = 128
BLOCK = 2 * HEAD_DIM
WAIT_QUARTERS = 3
HELD = 2
MESH = pl.DeviceIdType.MESH

query_scale = 144.0 ** (-0.5)


def each(start, stop, body):
    if stop - start == 1:
        body(start)
    elif stop > start:
        lax.fori_loop(start, stop, lambda i, _: (body(i), None)[1], None)


def kernel(
    n, grp, pos_ref, freq_ref, gain_ref, tok_ref, q_ref, k_ref, v_ref, out_ref,
    wbuf, normed, kvbuf, posbuf, qbuf, acc, cos_ref, sin_ref, qpos_ref,
    tok_sem, own_sem, x_send, x_recv, y_send, y_recv, s_send, s_recv, t_send, t_recv,
    kv_send, kv_recv, pos_send, pos_recv,
):
    c = lax.axis_index("ctx")
    g = lax.axis_index("grp")
    pairs = grp // 2
    near = g % 2
    pair = g // 2
    sibling = pair * 2 + (1 - near)
    depth = q_ref.shape[0]
    part = depth // grp
    rows = tok_ref.shape[0]
    kv_blocks = k_ref.shape[1] // BLOCK
    groups = k_ref.shape[1] // HEAD_DIM
    q_blocks = q_ref.shape[1] // BLOCK
    sources = [(k_ref, i) for i in range(kv_blocks)]
    sources += [(v_ref, i) for i in range(kv_blocks)]
    sources += [(q_ref, i) for i in range(q_blocks)]
    blocks = len(sources)

    def region(owner, member):
        return pl.ds(pl.multiple_of(owner * depth + member * part, 16), part)

    def peer(d):
        return lax.rem(c + d, n)

    def source(d):
        return lax.rem(c + n - d, n)

    def far(j):
        return lax.rem(pair + j, pairs)

    def near_of(j):
        return lax.rem(pair + pairs - j, pairs)

    def x_copy(b, d):
        return pltpu.make_async_remote_copy(
            src_ref=wbuf.at[b, region(c, g)], dst_ref=wbuf.at[b, region(c, g)],
            send_sem=x_send.at[b, d - 1], recv_sem=x_recv.at[b, d - 1],
            device_id={"ctx": peer(d)}, device_id_type=MESH,
        )

    def hop(b, where, send, recv, member):
        return pltpu.make_async_remote_copy(
            src_ref=wbuf.at[b, where], dst_ref=wbuf.at[b, where],
            send_sem=send, recv_sem=recv, device_id={"grp": member}, device_id_type=MESH,
        )

    def y_copy(b, d, j):
        return hop(b, region(source(d), g), y_send.at[b, d - 1, j - 1], y_recv.at[b, d - 1, j - 1],
                   far(j) * 2 + near)

    def y_wait(b, d, j):
        hop(b, region(source(d), near_of(j) * 2 + near), y_send.at[b, d - 1, j - 1],
            y_recv.at[b, d - 1, j - 1], sibling).wait_recv()

    def s_copy(b, d):
        return hop(b, region(source(d), g), s_send.at[b, d - 1], s_recv.at[b, d - 1], sibling)

    def s_wait(b, d):
        hop(b, region(source(d), sibling), s_send.at[b, d - 1], s_recv.at[b, d - 1],
            sibling).wait_recv()

    def t_copy(b, d, j):
        return hop(b, region(source(d), near_of(j) * 2 + near), t_send.at[b, d - 1, j - 1],
                   t_recv.at[b, d - 1, j - 1], sibling)

    def t_wait(b, d, j):
        hop(b, region(source(d), near_of(j) * 2 + 1 - near), t_send.at[b, d - 1, j - 1],
            t_recv.at[b, d - 1, j - 1], sibling).wait_recv()

    def kv_copy(b, d, owner):
        return pltpu.make_async_remote_copy(
            src_ref=kvbuf.at[b, owner], dst_ref=kvbuf.at[b, owner],
            send_sem=kv_send.at[b, d - 1], recv_sem=kv_recv.at[b, d - 1],
            device_id={"ctx": peer(d)}, device_id_type=MESH,
        )

    def pos_copy(d, owner):
        return pltpu.make_async_remote_copy(
            src_ref=posbuf.at[owner], dst_ref=posbuf.at[owner],
            send_sem=pos_send.at[d - 1], recv_sem=pos_recv.at[d - 1],
            device_id={"ctx": peer(d)}, device_id_type=MESH,
        )

    def own_copy(b):
        ref, col = sources[b]
        return pltpu.make_async_copy(
            ref.at[:, pl.ds(col * BLOCK, BLOCK)],
            wbuf.at[b, pl.ds(pl.multiple_of(c * depth, 16), depth)], own_sem.at[b],
        )

    tok_copy = pltpu.make_async_copy(tok_ref, normed, tok_sem)
    own_copy(0).start()
    own_copy(1).start()
    tok_copy.start()
    for b in range(2, blocks):
        own_copy(b).start()

    barrier = pltpu.get_barrier_semaphore()

    def greet(**where):
        pl.semaphore_signal(barrier, inc=1, device_id=where, device_id_type=MESH)

    each(1, n, lambda d: greet(ctx=peer(d)))
    each(1, pairs, lambda j: greet(grp=far(j) * 2 + near))
    greet(grp=sibling)
    pl.semaphore_wait(barrier, n - 1 + pairs - 1 + 1)

    def send_block(b):
        own_copy(b).wait()
        each(1, n, lambda d: x_copy(b, d).start())

    send_block(0)
    send_block(1)

    lanes = pos_ref[...][None, :]
    posbuf[c] = jnp.broadcast_to(lanes, posbuf.shape[1:])
    qpos = jnp.transpose(
        jnp.broadcast_to(lanes.astype(jnp.float32), (HEAD_DIM, rows)), (1, 0)
    )
    qpos_ref[...] = qpos
    angle = qpos * freq_ref[...]
    lane = lax.broadcasted_iota(jnp.int32, angle.shape, 1)
    sine = jnp.sin(angle)
    cos_ref[...] = jnp.cos(angle)
    sin_ref[...] = jnp.where(lane < HEAD_DIM // 2, -sine, sine)

    tok_copy.wait()
    strip = 32

    def norm_rows(i):
        where = pl.ds(pl.multiple_of(i * strip, strip), strip)
        inputs = normed[where, :].astype(jnp.float32)
        mean = jnp.mean(inputs * inputs, -1, keepdims=True)
        normed[where, :] = (inputs * lax.rsqrt(mean + 1e-06) * gain_ref[...][None, :]).astype(jnp.bfloat16)

    each(0, rows // strip, norm_rows)

    tall = math.gcd(rows, 256)

    def project(b, store, rope, scale):
        def tile(i):
            where = pl.ds(pl.multiple_of(i * tall, tall), tall)
            field = jnp.dot(normed[where, :], wbuf[b], preferred_element_type=jnp.float32)
            if rope:
                cosine, sine = cos_ref[where, :], sin_ref[where, :]
                halves = []
                for h in range(2):
                    one = field[:, h * HEAD_DIM : (h + 1) * HEAD_DIM]
                    halves.append(one * cosine + pltpu.roll(one, HEAD_DIM // 2, 1) * sine)
                field = jnp.concatenate(halves, -1)
            if scale is not None:
                field = field * scale
            store(where, field.astype(jnp.bfloat16))

        each(0, rows // tall, tile)

    def attend(b, owner, first, last):
        def tile(i):
            where = pl.ds(pl.multiple_of(i * tall, tall), tall)
            keys = kvbuf[b, owner]
            values = kvbuf[groups + b, owner]
            values = jnp.concatenate([values, jnp.ones_like(values)], -1)
            key_pos = posbuf[owner, 0:1, :].astype(jnp.float32)
            allowed = key_pos <= qpos_ref[where, 0:1]
            for h in range(2):
                cols = pl.ds(h * HEAD_DIM, HEAD_DIM)
                scores = lax.dot_general(
                    qbuf[b, where, cols], keys, (((1,), (1,)), ((), ())),
                    preferred_element_type=jnp.float32,
                )
                capped = jnp.tanh(scores * (1.0 / 50.0)) * (50.0 * math.log2(math.e))
                weights = jnp.where(allowed, jnp.exp2(capped), 0.0).astype(jnp.bfloat16)
                both = jnp.dot(weights, values, preferred_element_type=jnp.float32)
                if not first:
                    both = both + acc[b, h, where, :]
                if last:
                    done = both[:, :HEAD_DIM] / both[:, HEAD_DIM:]
                    out_ref[where, pl.ds(b * BLOCK + h * HEAD_DIM, HEAD_DIM)] = done.astype(
                        out_ref.dtype
                    )
                else:
                    acc[b, h, where, :] = both

        each(0, rows // tall, tile)

    received = set()

    def attend_others(b):
        if "pos" not in received:
            received.add("pos")
            each(1, n, lambda d: pos_copy(d, source(d)).wait_recv())
        for index in (b, groups + b):
            if index not in received:
                received.add(index)
                each(1, n, lambda d: kv_copy(index, d, source(d)).wait_recv())
        each(1, n - 1, lambda d: attend(b, source(d), False, False))
        attend(b, source(n - 1), False, True)

    def send_group(h):
        each(1, n, lambda d: kv_copy(h, d, c).start())
        each(1, n, lambda d: kv_copy(groups + h, d, c).start())

    def store_kv(first):
        def store(where, field):
            kvbuf[first, c, where, :] = field[:, :HEAD_DIM]
            kvbuf[first + 1, c, where, :] = field[:, HEAD_DIM:]

        return store

    def store_q(h):
        def store(where, field):
            qbuf[h, where, :] = field

        return store

    for t in range(blocks + 2):
        if t < blocks:
            def forward(d, b=t):
                x_copy(b, d).wait_recv()
                each(1, pairs, lambda j: y_copy(b, d, j).start())
                s_copy(b, d).start()

            each(1, n, forward)
        if 1 <= t <= blocks:
            def onward(d, b=t - 1):
                def one(j):
                    y_wait(b, d, j)
                    t_copy(b, d, j).start()

                each(1, pairs, one)

            each(1, n, onward)
        if t >= 2:
            b = t - 2

            def arrive(d, b=b):
                s_wait(b, d)
                each(1, pairs, lambda j: t_wait(b, d, j))

            each(1, n, arrive)
            if b < 2 * kv_blocks:
                project(b, store_kv(2 * b), b < kv_blocks, None)
        if t + 2 < blocks:
            send_block(t + 2)
        if t == 2:
            each(1, n, lambda d: pos_copy(d, c).start())
        if t >= blocks - 2:
            share = [h for h in range(groups) if min(blocks - 2 + h, blocks) == t]
            for h in share:
                send_group(h)
        if t >= 2 and t - 2 >= 2 * kv_blocks:
            h = t - 2 - 2 * kv_blocks
            project(t - 2, store_q(h), True, query_scale)
            attend(h, c, True, False)
            if t == blocks:
                attend_others(0)
    for h in range(1, q_blocks):
        attend_others(h)

    def settle(d):
        pos_copy(d, c).wait_send()
        for b in range(2 * groups):
            kv_copy(b, d, c).wait_send()
        for b in range(blocks):
            x_copy(b, d).wait_send()
            s_copy(b, d).wait_send()

            def pair_sends(j, b=b):
                y_copy(b, d, j).wait_send()
                t_copy(b, d, j).wait_send()

            each(1, pairs, pair_sends)

    each(1, n, settle)


def write_out(in_ref, out_ref, sem):
    copy = pltpu.make_async_copy(in_ref, out_ref, sem)
    copy.start()
    copy.wait()


def on_device(n, grp, tokens, token_pos, norm_gain, query_weight, key_weight, value_weight):
    rows, width = tokens.shape
    depth, q_cols = query_weight.shape
    kv_cols = key_weight.shape[1]
    q_blocks, kv_blocks = q_cols // BLOCK, kv_cols // BLOCK
    blocks = q_blocks + 2 * kv_blocks
    pairs = grp // 2
    half = HEAD_DIM // 2
    freq = 10000.0 ** (-np.arange(half) * 2.0 / HEAD_DIM)
    freq = np.concatenate([freq, freq])[None, :].astype(np.float32)
    dma = pltpu.SemaphoreType.DMA
    far = max(pairs - 1, 1)
    vmem = pl.BlockSpec(memory_space=pltpu.VMEM)
    anywhere = pl.BlockSpec(memory_space=pl.ANY)
    held = [pltpu.with_memory_space_constraint(x, pltpu.HBM) for x in (tokens, query_weight, key_weight, value_weight)]
    attended = pl.pallas_call(
        functools.partial(kernel, n, grp),
        out_shape=pltpu.VMEM((rows, q_cols), jnp.bfloat16),
        in_specs=[vmem] * 3 + [pl.BlockSpec(memory_space=pltpu.HBM)] * 4,
        out_specs=vmem,
        scratch_shapes=[
            pltpu.VMEM((blocks, n * depth, BLOCK), jnp.bfloat16),
            pltpu.VMEM((rows, width), jnp.bfloat16),
            pltpu.VMEM((4 * kv_blocks, n, rows, HEAD_DIM), jnp.bfloat16),
            pltpu.VMEM((n, 8, rows), jnp.int32),
            pltpu.VMEM((q_blocks, rows, BLOCK), jnp.bfloat16),
            pltpu.VMEM((q_blocks, 2, rows, BLOCK), jnp.float32),
            pltpu.VMEM((rows, HEAD_DIM), jnp.float32),
            pltpu.VMEM((rows, HEAD_DIM), jnp.float32),
            pltpu.VMEM((rows, HEAD_DIM), jnp.float32),
            dma(()),
            dma((blocks,)),
            dma((blocks, n - 1)),
            dma((blocks, n - 1)),
            dma((blocks, n - 1, far)),
            dma((blocks, n - 1, far)),
            dma((blocks, n - 1)),
            dma((blocks, n - 1)),
            dma((blocks, n - 1, far)),
            dma((blocks, n - 1, far)),
            dma((4 * kv_blocks, n - 1)),
            dma((4 * kv_blocks, n - 1)),
            dma((n - 1,)),
            dma((n - 1,)),
        ],
        compiler_params=pltpu.CompilerParams(
            collective_id=0, has_side_effects=True, vmem_limit_bytes=44 * 1024 * 1024
        ),
    )(token_pos, freq, norm_gain, *held)
    return pl.pallas_call(
        write_out,
        out_shape=jax.ShapeDtypeStruct(attended.shape, attended.dtype),
        in_specs=[vmem],
        out_specs=anywhere,
        scratch_shapes=[dma(())],
        compiler_params=pltpu.CompilerParams(vmem_limit_bytes=4 * 1024 * 1024),
    )(attended)


def pair_kernel(
    line, pos_ref, freq_ref, gain_ref, tok_ref, q_ref, k_ref, v_ref, out_ref,
    xbuf, oth, near, wbuf, psend, precv, acc, kbuf, vbuf, qbuf, obuf, cos_ref, sin_ref, qpos_ref,
    factor_ref, kpos_ref, side, pos_in, freq_in, gain_in, gain_row,
    tok_sem, w_sem, in_sem, side_send, side_recv, x_send, x_recv, up_send, up_recv, dn_send, dn_recv,
    p_send, p_recv, r_send, r_recv, o_send, o_recv,
):
    c = lax.axis_index("ctx")
    z = lax.axis_index("tp")
    o = 1 - c
    first = lax.axis_index("grp") % 2 == 0
    rows, half = oth.shape
    heads = wbuf.shape[0]
    mine = heads // 2
    quarter = rows // line
    subs = x_recv.shape[0]
    strip = quarter // subs
    tall = math.gcd(rows, 256)
    tiles = rows // tall
    last = line - 1

    def at_least(k):
        return (z + line - k) // line

    order = [sorted(range(line), key=lambda q, k=k: (abs(q - k), q)) for k in range(line)]

    def stage_quarter(s):
        q = order[0][s]
        for k in range(1, line):
            q = q + (order[k][s] - order[k - 1][s]) * at_least(k)
        return q

    def band(q, i=0, size=quarter):
        return pl.ds(pl.multiple_of(q * quarter + i * size, strip), size)

    def columns(side, i, width):
        return pl.ds(pl.multiple_of((side * mine + i) * width, HEAD_DIM), width)

    def features(side):
        return pl.ds(pl.multiple_of(side * half, HEAD_DIM), half)

    def w_copies(s):
        side, i = (o, s) if s < mine else (c, s - mine)
        parts = [
            (k_ref, HEAD_DIM, 0), (v_ref, HEAD_DIM, HEAD_DIM), (q_ref, BLOCK, 2 * HEAD_DIM),
        ]
        return [
            pltpu.make_async_copy(
                ref.at[:, columns(side, i, width)], wbuf.at[s, :, pl.ds(at, width)], w_sem.at[s]
            )
            for ref, width, at in parts
        ]

    own_tokens = pltpu.make_async_copy(tok_ref.at[:, features(c)], xbuf.at[0], tok_sem.at[0])

    def other_tokens(j):
        where = band(lax.rem(z + j, line))
        return pltpu.make_async_copy(tok_ref.at[where, features(o)], oth.at[where], tok_sem.at[min(j + 1, 2)])

    def start(copies):
        for copy in copies:
            copy.start()

    def wait(copies):
        for copy in copies:
            copy.wait()

    def remote(src, dst, send, recv, **where):
        return pltpu.make_async_remote_copy(
            src_ref=src, dst_ref=dst, send_sem=send, recv_sem=recv,
            device_id=where, device_id_type=MESH,
        )

    def x_copy(i):
        where = band(z, i, strip)
        return remote(oth.at[where], xbuf.at[1, where], x_send, x_recv.at[i], ctx=o)

    def up_copy(e, hops):
        where = band(z - hops - e // subs, e % subs, strip)
        return remote(xbuf.at[1, where], xbuf.at[1, where], up_send.at[e // subs], up_recv.at[e], tp=z + 1 - 2 * hops)

    def dn_copy(e, hops):
        where = band(z + hops + e // subs, e % subs, strip)
        return remote(xbuf.at[1, where], xbuf.at[1, where], dn_send.at[e // subs], dn_recv.at[e], tp=z - 1 + 2 * hops)

    pieces = rows // HEAD_DIM

    def pack(first, row):
        for k in range(pieces):
            side[0, first + k : first + k + 1, :] = row[:, k * HEAD_DIM : (k + 1) * HEAD_DIM]

    def unpack(slot, first):
        return jnp.concatenate([side[slot, first + k : first + k + 1, :] for k in range(pieces)], -1)

    def sent(ref, sem):
        remote(ref, ref, sem, sem, ctx=o).wait_send()

    def arrived(ref, sem):
        remote(ref, ref, sem, sem, ctx=o).wait_recv()

    def side_copy():
        return remote(side.at[0], side.at[1], side_send, side_recv, ctx=o)

    def p_copy(i, t):
        where = pl.ds(t * tall, tall)
        return remote(psend.at[0, i, where], precv.at[1, i, where], p_send.at[i], p_recv.at[i], ctx=o)

    def r_copy(i, s):
        where = band(stage_quarter(s))
        return remote(psend.at[1, i, where], precv.at[0, i, where], r_send.at[i], r_recv.at[i], ctx=o)

    def o_copy(i, t, side):
        where = pl.ds(t * tall, tall)
        return remote(
            obuf.at[i, where], out_ref.at[where, columns(side, i, BLOCK)], o_send, o_recv, ctx=o
        )

    small = [
        pltpu.make_async_copy(gain_ref, gain_in, in_sem.at[0]),
        pltpu.make_async_copy(pos_ref, pos_in, in_sem.at[1]),
        pltpu.make_async_copy(freq_ref, freq_in, in_sem.at[2]),
    ]
    other_tokens(0).start()
    start(small)

    barrier = pltpu.get_barrier_semaphore()

    def greet(**where):
        pl.semaphore_signal(barrier, inc=1, device_id=where, device_id_type=MESH)

    greet(ctx=o)

    @pl.when(z > 0)
    def _():
        greet(tp=z - 1)

    @pl.when(z < last)
    def _():
        greet(tp=z + 1)

    own_tokens.start()
    for j in range(1, line):
        other_tokens(j).start()
    other_tokens(0).wait()
    pl.semaphore_wait(barrier, 1 + at_least(1) + 1 - at_least(last))

    @pl.when(first)
    def _():
        for i in range(subs):
            x_copy(i).start()

    for s in range(heads):
        start(w_copies(s))

    vbuf[...] = jnp.ones_like(vbuf)
    wait(small)
    gain_row[...] = gain_in[...][None, :]
    pack(0, pos_in[...][None, :].astype(jnp.float32))

    def norm_rows(where):
        own = xbuf[0, where, :].astype(jnp.float32)
        other = oth[where, :].astype(jnp.float32)
        total = jnp.sum(own * own, -1, keepdims=True) + jnp.sum(other * other, -1, keepdims=True)
        factor = lax.rsqrt(total * (1.0 / (2 * half)) + 1e-06)
        factor_ref[where, :] = jnp.broadcast_to(factor, (strip, HEAD_DIM))
        xbuf[0, where, :] = (own * factor * gain_row[:, features(c)]).astype(jnp.bfloat16)

    def norm_quarter(j):
        if j == 0:
            own_tokens.wait()
        if j == 1:
            rest = oth.at[pl.ds(0, rows - quarter)]
            pltpu.make_async_copy(rest, rest, tok_sem.at[2]).wait()
        each(0, subs, lambda i: norm_rows(band(lax.rem(z + j, line), i, strip)))

    def norm_far(q):
        def one(i):
            where = band(q, i, strip)
            raw = xbuf[1, where, :].astype(jnp.float32)
            normed = raw * factor_ref[where, 0:1] * gain_row[:, features(c)]
            near[pl.ds(pl.multiple_of(i * strip, strip), strip), :] = normed.astype(jnp.bfloat16)

        each(0, subs, one)

    def product(rows_in, s):
        return jnp.dot(rows_in, wbuf[s], preferred_element_type=jnp.float32)

    def tile(t):
        return pl.ds(pl.multiple_of(t * tall, tall), tall)

    loaded = set()

    def load(s):
        if s not in loaded:
            loaded.add(s)
            pltpu.make_async_copy(wbuf.at[s], wbuf.at[s], w_sem.at[s]).wait()

    def own_product(i):
        load(i)

        def one(t):
            psend[0, i, tile(t), :] = product(xbuf[0, tile(t), :], i).astype(jnp.bfloat16)

        each(0, tiles, one)
        for t in range(tiles):
            p_copy(i, t).start()

    def own_local(i):
        load(mine + i)

        def one(t):
            acc[0, i, tile(t), :] = product(xbuf[0, tile(t), :], mine + i)

        each(0, tiles, one)

    def far_product(i, s):
        load(i)
        where = band(stage_quarter(s))
        psend[1, i, where, :] = product(near[...], i).astype(jnp.bfloat16)

    def far_local(i, s):
        load(mine + i)
        where = band(stage_quarter(s))
        acc[1, i, where, :] = product(near[...], mine + i)

    def angles(slot):
        where = pl.ds(slot * rows, rows)
        lanes = unpack(slot, 0)
        kpos_ref[:, where] = jnp.broadcast_to(lanes, (8, rows))
        qpos = jnp.transpose(jnp.broadcast_to(lanes, (HEAD_DIM, rows)), (1, 0))
        qpos_ref[where, :] = qpos
        angle = qpos * freq_in[...]
        lane = lax.broadcasted_iota(jnp.int32, angle.shape, 1)
        sine = jnp.sin(angle)
        cos_ref[where, :] = jnp.cos(angle)
        sin_ref[where, :] = jnp.where(lane < HEAD_DIM // 2, -sine, sine)

    def finish(i, slot):
        def one(t):
            where = tile(t)
            at = pl.ds(pl.multiple_of(slot * rows + t * tall, tall), tall)
            field = acc[slot, i, where, :] + precv[slot, i, where, :].astype(jnp.float32)
            cosine, sine = cos_ref[at, :], sin_ref[at, :]

            def rope(x):
                return x * cosine + pltpu.roll(x, HEAD_DIM // 2, 1) * sine

            kbuf[i, at, :] = rope(field[:, :HEAD_DIM]).astype(jnp.bfloat16)
            vbuf[i, at, :HEAD_DIM] = field[:, HEAD_DIM : 2 * HEAD_DIM].astype(jnp.bfloat16)
            for h in range(2):
                one = field[:, (2 + h) * HEAD_DIM : (3 + h) * HEAD_DIM]
                qbuf[i, at, h * HEAD_DIM : (h + 1) * HEAD_DIM] = (rope(one) * query_scale).astype(jnp.bfloat16)

        each(0, tiles, one)

    def attend(i, slot, t, store):
        at = pl.ds(pl.multiple_of(slot * rows + t * tall, tall), tall)
        for h in range(2):
            both = None
            for part in range(2):
                span = pl.ds(part * rows, rows)
                scores = lax.dot_general(
                    qbuf[i, at, h * HEAD_DIM : (h + 1) * HEAD_DIM], kbuf[i, span, :],
                    (((1,), (1,)), ((), ())), preferred_element_type=jnp.float32,
                )
                allowed = kpos_ref[0:1, span] <= qpos_ref[at, 0:1]
                capped = jnp.tanh(scores * (1.0 / 50.0)) * (50.0 * math.log2(math.e))
                weights = jnp.where(allowed, jnp.exp2(capped), 0.0).astype(jnp.bfloat16)
                more = jnp.dot(weights, vbuf[i, span, :], preferred_element_type=jnp.float32)
                both = more if both is None else both + more
            done = (both[:, :HEAD_DIM] / both[:, HEAD_DIM:]).astype(jnp.bfloat16)
            store(h, done)

    def attend_far(i):
        for t in range(tiles):
            def store(h, done, t=t):
                obuf[i, t * tall : (t + 1) * tall, h * HEAD_DIM : (h + 1) * HEAD_DIM] = done

            attend(i, 1, t, store)
            o_copy(i, t, c).start()

    def attend_own(i):
        def one(t):
            def store(h, done):
                out_ref[tile(t), pl.ds(pl.multiple_of((c * mine + i) * BLOCK + h * HEAD_DIM, HEAD_DIM), HEAD_DIM)] = done

            attend(i, 0, t, store)

        each(0, tiles, one)

    def pass_on(r):
        if r < subs:
            x_copy(r).wait_recv()

            @pl.when(z < last)
            def _():
                up_copy(r, 0).start()

            @pl.when(z > 0)
            def _():
                dn_copy(r, 0).start()

        e = r - 1
        if 0 <= e < last * subs:
            @pl.when(z >= 1 + e // subs)
            def _():
                up_copy(e, 1).wait_recv()
                if e + subs < last * subs:
                    @pl.when(z < last)
                    def _():
                        up_copy(e + subs, 0).start()

            @pl.when(z + 1 + e // subs <= last)
            def _():
                dn_copy(e, 1).wait_recv()
                if e + subs < last * subs:
                    @pl.when(z > 0)
                    def _():
                        dn_copy(e + subs, 0).start()

    def stage(s):
        norm_far(stage_quarter(s))
        far_product(0, s)
        r_copy(0, s).start()
        for i in range(1, mine):
            far_product(i, s)
            early = line - HELD
            for done in range(early) if s == last - 1 else range(early, line) if s == last else ():
                r_copy(i, done).start()
        for i in range(mine):
            far_local(i, s)

    def far_side():
        side_copy().wait_recv()
        lanes = jnp.broadcast_to(unpack(1, pieces), (HEAD_DIM, rows))
        factor_ref[...] = jnp.transpose(lanes, (1, 0))

    rounds = 1 + last * subs
    work = {r: [] for r in range(rounds)}
    stage_at = [subs - 1] + [s * subs for s in range(1, line)]
    for s in range(line - 1):
        work[stage_at[s]].append(functools.partial(stage, s))
    work[stage_at[0]].insert(0, far_side)
    fill = [functools.partial(own_product, i) for i in range(mine)]
    fill += [functools.partial(angles, 0)]
    fill += [functools.partial(own_local, i) for i in range(mine)]
    fill += [functools.partial(angles, 1)]

    for j in range(line):
        norm_quarter(j)
        if j == WAIT_QUARTERS - 1:
            @pl.when(jnp.logical_not(first))
            def _():
                for i in range(subs):
                    x_copy(i).start()

    pack(pieces, jnp.transpose(factor_ref[...], (1, 0))[0:1, :])
    side_copy().start()
    for r in range(rounds):
        pass_on(r)
        if work[r]:
            for task in work[r]:
                task()
        elif fill:
            fill.pop(0)()
    for task in fill:
        task()

    stage(last)
    for i in range(mine):
        arrived(precv.at[1, i], p_recv.at[i])
        finish(i, 1)
    for i in range(mine):
        arrived(precv.at[0, i], r_recv.at[i])
        finish(i, 0)
        attend_far(i)
        attend_own(i)
    arrived(obuf, o_recv)

    side_copy().wait_send()
    sent(xbuf.at[1, band(z)], x_send)
    for k in range(last):
        @pl.when((z < last) & (z >= k))
        def _(k=k):
            sent(xbuf.at[1, band(z - k)], up_send.at[k])

        @pl.when((z > 0) & (z + k <= last))
        def _(k=k):
            sent(xbuf.at[1, band(z + k)], dn_send.at[k])

    for i in range(mine):
        sent(psend.at[0, i], p_send.at[i])
        sent(psend.at[1, i], r_send.at[i])
    sent(obuf, o_send)


def rope_freq():
    half = HEAD_DIM // 2
    freq = 10000.0 ** (-np.arange(half) * 2.0 / HEAD_DIM)
    return np.concatenate([freq, freq])[None, :].astype(np.float32)


def on_pair(line, tokens, token_pos, norm_gain, query_weight, key_weight, value_weight):
    rows, width = tokens.shape
    depth, q_cols = query_weight.shape
    heads = key_weight.shape[1] // HEAD_DIM
    mine = heads // 2
    subs = max(rows // line // 32, 1)
    dma = pltpu.SemaphoreType.DMA
    vmem = pl.BlockSpec(memory_space=pltpu.VMEM)
    hbm = pl.BlockSpec(memory_space=pltpu.HBM)
    ins = (token_pos, jnp.asarray(rope_freq()), norm_gain, tokens, query_weight, key_weight, value_weight)
    held = [pltpu.with_memory_space_constraint(x, pltpu.HBM) for x in ins]
    bf16, f32 = jnp.bfloat16, jnp.float32
    along = max((line - 1) * subs, 1)
    attended = pl.pallas_call(
        functools.partial(pair_kernel, line),
        out_shape=pltpu.VMEM((rows, q_cols), bf16),
        in_specs=[hbm] * 7,
        out_specs=vmem,
        scratch_shapes=[
            pltpu.VMEM((2, rows, depth), bf16),
            pltpu.VMEM((rows, depth), bf16),
            pltpu.VMEM((rows // line, depth), bf16),
            pltpu.VMEM((heads, depth, 2 * BLOCK), bf16),
            pltpu.VMEM((2, mine, rows, 2 * BLOCK), bf16),
            pltpu.VMEM((2, mine, rows, 2 * BLOCK), bf16),
            pltpu.VMEM((2, mine, rows, 2 * BLOCK), f32),
            pltpu.VMEM((mine, 2 * rows, HEAD_DIM), bf16),
            pltpu.VMEM((mine, 2 * rows, BLOCK), bf16),
            pltpu.VMEM((mine, 2 * rows, BLOCK), bf16),
            pltpu.VMEM((mine, rows, BLOCK), bf16),
            pltpu.VMEM((2 * rows, HEAD_DIM), f32),
            pltpu.VMEM((2 * rows, HEAD_DIM), f32),
            pltpu.VMEM((2 * rows, HEAD_DIM), f32),
            pltpu.VMEM((rows, HEAD_DIM), f32),
            pltpu.VMEM((8, 2 * rows), f32),
            pltpu.VMEM((2, 2 * rows // HEAD_DIM, HEAD_DIM), f32),
            pltpu.VMEM((rows,), jnp.int32),
            pltpu.VMEM((1, HEAD_DIM), f32),
            pltpu.VMEM((width,), f32),
            pltpu.VMEM((1, width), f32),
            dma((3,)),
            dma((heads,)),
            dma((3,)),
            dma(()),
            dma(()),
            dma(()),
            dma((subs,)),
            dma((line - 1,)),
            dma((along,)),
            dma((line - 1,)),
            dma((along,)),
            dma((mine,)),
            dma((mine,)),
            dma((mine,)),
            dma((mine,)),
            dma(()),
            dma(()),
        ],
        compiler_params=pltpu.CompilerParams(
            collective_id=0, has_side_effects=True, vmem_limit_bytes=44 * 1024 * 1024
        ),
    )(*held)
    return attended


def solution(mesh):
    in_specs = (
        P(("grp", "ctx"), None),
        P(("grp", "ctx")),
        P(),
        P("ctx", "tp"),
        P("ctx", "tp"),
        P("ctx", "tp"),
    )
    out_specs = P(("grp", "ctx"), "tp")
    ctx, grp, line = (mesh.shape[name] for name in ("ctx", "grp", "tp"))

    def local(tokens, token_pos, norm_gain, query_weight, key_weight, value_weight):
        rows, width = tokens.shape
        depth, kv_cols = key_weight.shape
        heads = kv_cols // HEAD_DIM
        paired = ctx == 2 and width == 2 * depth and heads % 2 == 0
        paired = paired and line > 1 and rows % (line * 32) == 0 and rows % HEAD_DIM == 0
        plan = functools.partial(on_pair, line) if paired else functools.partial(on_device, ctx, grp)
        return plan(tokens, token_pos, norm_gain, query_weight, key_weight, value_weight)

    return jax.shard_map(
        local, mesh=mesh, in_specs=in_specs, out_specs=out_specs, check_vma=False,
    )
```

```python
import functools
import math

import jax
import jax.numpy as jnp
import numpy as np
from jax import lax
from jax.experimental import pallas as pl
from jax.experimental.pallas import tpu as pltpu
from jax.sharding import PartitionSpec as P

HEAD_DIM = 128
BLOCK = 2 * HEAD_DIM
WAIT_QUARTERS = 3
HELD = 1
MESH = pl.DeviceIdType.MESH

query_scale = 144.0 ** (-0.5)


def each(start, stop, body):
    if stop - start == 1:
        body(start)
    elif stop > start:
        lax.fori_loop(start, stop, lambda i, _: (body(i), None)[1], None)


def kernel(
    n, grp, pos_ref, freq_ref, gain_ref, tok_ref, q_ref, k_ref, v_ref, out_ref,
    wbuf, normed, kvbuf, posbuf, qbuf, acc, cos_ref, sin_ref, qpos_ref,
    tok_sem, own_sem, x_send, x_recv, y_send, y_recv, s_send, s_recv, t_send, t_recv,
    kv_send, kv_recv, pos_send, pos_recv,
):
    c = lax.axis_index("ctx")
    g = lax.axis_index("grp")
    pairs = grp // 2
    near = g % 2
    pair = g // 2
    sibling = pair * 2 + (1 - near)
    depth = q_ref.shape[0]
    part = depth // grp
    rows = tok_ref.shape[0]
    kv_blocks = k_ref.shape[1] // BLOCK
    groups = k_ref.shape[1] // HEAD_DIM
    q_blocks = q_ref.shape[1] // BLOCK
    sources = [(k_ref, i) for i in range(kv_blocks)]
    sources += [(v_ref, i) for i in range(kv_blocks)]
    sources += [(q_ref, i) for i in range(q_blocks)]
    blocks = len(sources)

    def region(owner, member):
        return pl.ds(pl.multiple_of(owner * depth + member * part, 16), part)

    def peer(d):
        return lax.rem(c + d, n)

    def source(d):
        return lax.rem(c + n - d, n)

    def far(j):
        return lax.rem(pair + j, pairs)

    def near_of(j):
        return lax.rem(pair + pairs - j, pairs)

    def x_copy(b, d):
        return pltpu.make_async_remote_copy(
            src_ref=wbuf.at[b, region(c, g)], dst_ref=wbuf.at[b, region(c, g)],
            send_sem=x_send.at[b, d - 1], recv_sem=x_recv.at[b, d - 1],
            device_id={"ctx": peer(d)}, device_id_type=MESH,
        )

    def hop(b, where, send, recv, member):
        return pltpu.make_async_remote_copy(
            src_ref=wbuf.at[b, where], dst_ref=wbuf.at[b, where],
            send_sem=send, recv_sem=recv, device_id={"grp": member}, device_id_type=MESH,
        )

    def y_copy(b, d, j):
        return hop(b, region(source(d), g), y_send.at[b, d - 1, j - 1], y_recv.at[b, d - 1, j - 1],
                   far(j) * 2 + near)

    def y_wait(b, d, j):
        hop(b, region(source(d), near_of(j) * 2 + near), y_send.at[b, d - 1, j - 1],
            y_recv.at[b, d - 1, j - 1], sibling).wait_recv()

    def s_copy(b, d):
        return hop(b, region(source(d), g), s_send.at[b, d - 1], s_recv.at[b, d - 1], sibling)

    def s_wait(b, d):
        hop(b, region(source(d), sibling), s_send.at[b, d - 1], s_recv.at[b, d - 1],
            sibling).wait_recv()

    def t_copy(b, d, j):
        return hop(b, region(source(d), near_of(j) * 2 + near), t_send.at[b, d - 1, j - 1],
                   t_recv.at[b, d - 1, j - 1], sibling)

    def t_wait(b, d, j):
        hop(b, region(source(d), near_of(j) * 2 + 1 - near), t_send.at[b, d - 1, j - 1],
            t_recv.at[b, d - 1, j - 1], sibling).wait_recv()

    def kv_copy(b, d, owner):
        return pltpu.make_async_remote_copy(
            src_ref=kvbuf.at[b, owner], dst_ref=kvbuf.at[b, owner],
            send_sem=kv_send.at[b, d - 1], recv_sem=kv_recv.at[b, d - 1],
            device_id={"ctx": peer(d)}, device_id_type=MESH,
        )

    def pos_copy(d, owner):
        return pltpu.make_async_remote_copy(
            src_ref=posbuf.at[owner], dst_ref=posbuf.at[owner],
            send_sem=pos_send.at[d - 1], recv_sem=pos_recv.at[d - 1],
            device_id={"ctx": peer(d)}, device_id_type=MESH,
        )

    def own_copy(b):
        ref, col = sources[b]
        return pltpu.make_async_copy(
            ref.at[:, pl.ds(col * BLOCK, BLOCK)],
            wbuf.at[b, pl.ds(pl.multiple_of(c * depth, 16), depth)], own_sem.at[b],
        )

    tok_copy = pltpu.make_async_copy(tok_ref, normed, tok_sem)
    own_copy(0).start()
    own_copy(1).start()
    tok_copy.start()
    for b in range(2, blocks):
        own_copy(b).start()

    barrier = pltpu.get_barrier_semaphore()

    def greet(**where):
        pl.semaphore_signal(barrier, inc=1, device_id=where, device_id_type=MESH)

    each(1, n, lambda d: greet(ctx=peer(d)))
    each(1, pairs, lambda j: greet(grp=far(j) * 2 + near))
    greet(grp=sibling)
    pl.semaphore_wait(barrier, n - 1 + pairs - 1 + 1)

    def send_block(b):
        own_copy(b).wait()
        each(1, n, lambda d: x_copy(b, d).start())

    send_block(0)
    send_block(1)

    lanes = pos_ref[...][None, :]
    posbuf[c] = jnp.broadcast_to(lanes, posbuf.shape[1:])
    qpos = jnp.transpose(
        jnp.broadcast_to(lanes.astype(jnp.float32), (HEAD_DIM, rows)), (1, 0)
    )
    qpos_ref[...] = qpos
    angle = qpos * freq_ref[...]
    lane = lax.broadcasted_iota(jnp.int32, angle.shape, 1)
    sine = jnp.sin(angle)
    cos_ref[...] = jnp.cos(angle)
    sin_ref[...] = jnp.where(lane < HEAD_DIM // 2, -sine, sine)

    tok_copy.wait()
    strip = 32

    def norm_rows(i):
        where = pl.ds(pl.multiple_of(i * strip, strip), strip)
        inputs = normed[where, :].astype(jnp.float32)
        mean = jnp.mean(inputs * inputs, -1, keepdims=True)
        normed[where, :] = (inputs * lax.rsqrt(mean + 1e-06) * gain_ref[...][None, :]).astype(jnp.bfloat16)

    each(0, rows // strip, norm_rows)

    tall = math.gcd(rows, 256)

    def project(b, store, rope, scale):
        def tile(i):
            where = pl.ds(pl.multiple_of(i * tall, tall), tall)
            field = jnp.dot(normed[where, :], wbuf[b], preferred_element_type=jnp.float32)
            if rope:
                cosine, sine = cos_ref[where, :], sin_ref[where, :]
                halves = []
                for h in range(2):
                    one = field[:, h * HEAD_DIM : (h + 1) * HEAD_DIM]
                    halves.append(one * cosine + pltpu.roll(one, HEAD_DIM // 2, 1) * sine)
                field = jnp.concatenate(halves, -1)
            if scale is not None:
                field = field * scale
            store(where, field.astype(jnp.bfloat16))

        each(0, rows // tall, tile)

    def attend(b, owner, first, last):
        def tile(i):
            where = pl.ds(pl.multiple_of(i * tall, tall), tall)
            keys = kvbuf[b, owner]
            values = kvbuf[groups + b, owner]
            values = jnp.concatenate([values, jnp.ones_like(values)], -1)
            key_pos = posbuf[owner, 0:1, :].astype(jnp.float32)
            allowed = key_pos <= qpos_ref[where, 0:1]
            for h in range(2):
                cols = pl.ds(h * HEAD_DIM, HEAD_DIM)
                scores = lax.dot_general(
                    qbuf[b, where, cols], keys, (((1,), (1,)), ((), ())),
                    preferred_element_type=jnp.float32,
                )
                capped = jnp.tanh(scores * (1.0 / 50.0)) * (50.0 * math.log2(math.e))
                weights = jnp.where(allowed, jnp.exp2(capped), 0.0).astype(jnp.bfloat16)
                both = jnp.dot(weights, values, preferred_element_type=jnp.float32)
                if not first:
                    both = both + acc[b, h, where, :]
                if last:
                    done = both[:, :HEAD_DIM] / both[:, HEAD_DIM:]
                    out_ref[where, pl.ds(b * BLOCK + h * HEAD_DIM, HEAD_DIM)] = done.astype(
                        out_ref.dtype
                    )
                else:
                    acc[b, h, where, :] = both

        each(0, rows // tall, tile)

    received = set()

    def attend_others(b):
        if "pos" not in received:
            received.add("pos")
            each(1, n, lambda d: pos_copy(d, source(d)).wait_recv())
        for index in (b, groups + b):
            if index not in received:
                received.add(index)
                each(1, n, lambda d: kv_copy(index, d, source(d)).wait_recv())
        each(1, n - 1, lambda d: attend(b, source(d), False, False))
        attend(b, source(n - 1), False, True)

    def send_group(h):
        each(1, n, lambda d: kv_copy(h, d, c).start())
        each(1, n, lambda d: kv_copy(groups + h, d, c).start())

    def store_kv(first):
        def store(where, field):
            kvbuf[first, c, where, :] = field[:, :HEAD_DIM]
            kvbuf[first + 1, c, where, :] = field[:, HEAD_DIM:]

        return store

    def store_q(h):
        def store(where, field):
            qbuf[h, where, :] = field

        return store

    for t in range(blocks + 2):
        if t < blocks:
            def forward(d, b=t):
                x_copy(b, d).wait_recv()
                each(1, pairs, lambda j: y_copy(b, d, j).start())
                s_copy(b, d).start()

            each(1, n, forward)
        if 1 <= t <= blocks:
            def onward(d, b=t - 1):
                def one(j):
                    y_wait(b, d, j)
                    t_copy(b, d, j).start()

                each(1, pairs, one)

            each(1, n, onward)
        if t >= 2:
            b = t - 2

            def arrive(d, b=b):
                s_wait(b, d)
                each(1, pairs, lambda j: t_wait(b, d, j))

            each(1, n, arrive)
            if b < 2 * kv_blocks:
                project(b, store_kv(2 * b), b < kv_blocks, None)
        if t + 2 < blocks:
            send_block(t + 2)
        if t == 2:
            each(1, n, lambda d: pos_copy(d, c).start())
        if t >= blocks - 2:
            share = [h for h in range(groups) if min(blocks - 2 + h, blocks) == t]
            for h in share:
                send_group(h)
        if t >= 2 and t - 2 >= 2 * kv_blocks:
            h = t - 2 - 2 * kv_blocks
            project(t - 2, store_q(h), True, query_scale)
            attend(h, c, True, False)
            if t == blocks:
                attend_others(0)
    for h in range(1, q_blocks):
        attend_others(h)

    def settle(d):
        pos_copy(d, c).wait_send()
        for b in range(2 * groups):
            kv_copy(b, d, c).wait_send()
        for b in range(blocks):
            x_copy(b, d).wait_send()
            s_copy(b, d).wait_send()

            def pair_sends(j, b=b):
                y_copy(b, d, j).wait_send()
                t_copy(b, d, j).wait_send()

            each(1, pairs, pair_sends)

    each(1, n, settle)


def write_out(in_ref, out_ref, sem):
    copy = pltpu.make_async_copy(in_ref, out_ref, sem)
    copy.start()
    copy.wait()


def on_device(n, grp, tokens, token_pos, norm_gain, query_weight, key_weight, value_weight):
    rows, width = tokens.shape
    depth, q_cols = query_weight.shape
    kv_cols = key_weight.shape[1]
    q_blocks, kv_blocks = q_cols // BLOCK, kv_cols // BLOCK
    blocks = q_blocks + 2 * kv_blocks
    pairs = grp // 2
    half = HEAD_DIM // 2
    freq = 10000.0 ** (-np.arange(half) * 2.0 / HEAD_DIM)
    freq = np.concatenate([freq, freq])[None, :].astype(np.float32)
    dma = pltpu.SemaphoreType.DMA
    far = max(pairs - 1, 1)
    vmem = pl.BlockSpec(memory_space=pltpu.VMEM)
    anywhere = pl.BlockSpec(memory_space=pl.ANY)
    held = [pltpu.with_memory_space_constraint(x, pltpu.HBM) for x in (tokens, query_weight, key_weight, value_weight)]
    attended = pl.pallas_call(
        functools.partial(kernel, n, grp),
        out_shape=pltpu.VMEM((rows, q_cols), jnp.bfloat16),
        in_specs=[vmem] * 3 + [pl.BlockSpec(memory_space=pltpu.HBM)] * 4,
        out_specs=vmem,
        scratch_shapes=[
            pltpu.VMEM((blocks, n * depth, BLOCK), jnp.bfloat16),
            pltpu.VMEM((rows, width), jnp.bfloat16),
            pltpu.VMEM((4 * kv_blocks, n, rows, HEAD_DIM), jnp.bfloat16),
            pltpu.VMEM((n, 8, rows), jnp.int32),
            pltpu.VMEM((q_blocks, rows, BLOCK), jnp.bfloat16),
            pltpu.VMEM((q_blocks, 2, rows, BLOCK), jnp.float32),
            pltpu.VMEM((rows, HEAD_DIM), jnp.float32),
            pltpu.VMEM((rows, HEAD_DIM), jnp.float32),
            pltpu.VMEM((rows, HEAD_DIM), jnp.float32),
            dma(()),
            dma((blocks,)),
            dma((blocks, n - 1)),
            dma((blocks, n - 1)),
            dma((blocks, n - 1, far)),
            dma((blocks, n - 1, far)),
            dma((blocks, n - 1)),
            dma((blocks, n - 1)),
            dma((blocks, n - 1, far)),
            dma((blocks, n - 1, far)),
            dma((4 * kv_blocks, n - 1)),
            dma((4 * kv_blocks, n - 1)),
            dma((n - 1,)),
            dma((n - 1,)),
        ],
        compiler_params=pltpu.CompilerParams(
            collective_id=0, has_side_effects=True, vmem_limit_bytes=44 * 1024 * 1024
        ),
    )(token_pos, freq, norm_gain, *held)
    return pl.pallas_call(
        write_out,
        out_shape=jax.ShapeDtypeStruct(attended.shape, attended.dtype),
        in_specs=[vmem],
        out_specs=anywhere,
        scratch_shapes=[dma(())],
        compiler_params=pltpu.CompilerParams(vmem_limit_bytes=4 * 1024 * 1024),
    )(attended)


def pair_kernel(
    line, pos_ref, freq_ref, gain_ref, tok_ref, q_ref, k_ref, v_ref, out_ref,
    xbuf, oth, near, wbuf, psend, precv, acc, kbuf, vbuf, qbuf, obuf, cos_ref, sin_ref, qpos_ref,
    factor_ref, kpos_ref, side, pos_in, freq_in, gain_in, gain_row,
    tok_sem, w_sem, in_sem, side_send, side_recv, x_send, x_recv, up_send, dn_send, z_recv,
    p_send, p_recv, r_recv, o_send, o_recv,
):
    c = lax.axis_index("ctx")
    z = lax.axis_index("tp")
    o = 1 - c
    first = lax.axis_index("grp") % 2 == 0
    rows, half = oth.shape
    heads = wbuf.shape[0]
    mine = heads // 2
    quarter = rows // line
    subs = x_recv.shape[0]
    strip = quarter // subs
    tall = math.gcd(rows, 256)
    tiles = rows // tall
    last = line - 1

    def at_least(k):
        return (z + line - k) // line

    order = [sorted(range(line), key=lambda q, k=k: (abs(q - k), q)) for k in range(line)]

    def stage_quarter(s):
        q = order[0][s]
        for k in range(1, line):
            q = q + (order[k][s] - order[k - 1][s]) * at_least(k)
        return q

    def band(q, i=0, size=quarter):
        return pl.ds(pl.multiple_of(q * quarter + i * size, strip), size)

    def columns(side, i, width):
        return pl.ds(pl.multiple_of((side * mine + i) * width, HEAD_DIM), width)

    def features(side):
        return pl.ds(pl.multiple_of(side * half, HEAD_DIM), half)

    def w_copies(s):
        side, i = (o, s) if s < mine else (c, s - mine)
        parts = [
            (k_ref, HEAD_DIM, 0), (v_ref, HEAD_DIM, HEAD_DIM), (q_ref, BLOCK, 2 * HEAD_DIM),
        ]
        return [
            pltpu.make_async_copy(
                ref.at[:, columns(side, i, width)], wbuf.at[s, :, pl.ds(at, width)], w_sem.at[s]
            )
            for ref, width, at in parts
        ]

    own_tokens = pltpu.make_async_copy(tok_ref.at[:, features(c)], xbuf.at[0], tok_sem.at[0])

    def other_tokens(j):
        where = band(lax.rem(z + j, line))
        return pltpu.make_async_copy(tok_ref.at[where, features(o)], oth.at[where], tok_sem.at[min(j + 1, 2)])

    def start(copies):
        for copy in copies:
            copy.start()

    def wait(copies):
        for copy in copies:
            copy.wait()

    def remote(src, dst, send, recv, **where):
        return pltpu.make_async_remote_copy(
            src_ref=src, dst_ref=dst, send_sem=send, recv_sem=recv,
            device_id=where, device_id_type=MESH,
        )

    def x_copy(i):
        where = band(z, i, strip)
        return remote(oth.at[where], xbuf.at[1, where], x_send, x_recv.at[i], ctx=o)

    def up_copy(e, hops):
        where = band(z - hops - e // subs, e % subs, strip)
        return remote(xbuf.at[1, where], xbuf.at[1, where], up_send.at[e // subs], z_recv.at[e], tp=z + 1 - 2 * hops)

    def dn_copy(e, hops):
        where = band(z + hops + e // subs, e % subs, strip)
        return remote(xbuf.at[1, where], xbuf.at[1, where], dn_send.at[e // subs], z_recv.at[last * subs - 1 - e], tp=z - 1 + 2 * hops)

    pieces = rows // HEAD_DIM

    def pack(first, row):
        for k in range(pieces):
            side[0, first + k : first + k + 1, :] = row[:, k * HEAD_DIM : (k + 1) * HEAD_DIM]

    def unpack(slot, first):
        return jnp.concatenate([side[slot, first + k : first + k + 1, :] for k in range(pieces)], -1)

    def sent(ref, sem):
        remote(ref, ref, sem, sem, ctx=o).wait_send()

    def arrived(ref, sem):
        remote(ref, ref, sem, sem, ctx=o).wait_recv()

    def side_copy():
        return remote(side.at[0], side.at[1], side_send, side_recv, ctx=o)

    def p_copy(i, t):
        where = pl.ds(t * tall, tall)
        return remote(psend.at[0, i, where], precv.at[1, i, where], p_send, p_recv.at[i], ctx=o)

    def r_copy(i, s):
        where = band(stage_quarter(s))
        return remote(psend.at[1, i, where], precv.at[0, i, where], p_send, r_recv.at[i], ctx=o)

    def o_copy(i, t, side):
        where = pl.ds(t * tall, tall)
        return remote(
            obuf.at[i, where], out_ref.at[where, columns(side, i, BLOCK)], o_send, o_recv, ctx=o
        )

    small = [
        pltpu.make_async_copy(gain_ref, gain_in, in_sem.at[0]),
        pltpu.make_async_copy(pos_ref, pos_in, in_sem.at[1]),
        pltpu.make_async_copy(freq_ref, freq_in, in_sem.at[2]),
    ]
    other_tokens(0).start()
    start(small)

    barrier = pltpu.get_barrier_semaphore()

    def greet(**where):
        pl.semaphore_signal(barrier, inc=1, device_id=where, device_id_type=MESH)

    greet(ctx=o)

    @pl.when(z > 0)
    def _():
        greet(tp=z - 1)

    @pl.when(z < last)
    def _():
        greet(tp=z + 1)

    own_tokens.start()
    for j in range(1, line):
        other_tokens(j).start()
    other_tokens(0).wait()
    pl.semaphore_wait(barrier, 1 + at_least(1) + 1 - at_least(last))

    @pl.when(first)
    def _():
        for i in range(subs):
            x_copy(i).start()

    for s in range(heads):
        start(w_copies(s))

    vbuf[...] = jnp.ones_like(vbuf)
    wait(small)
    gain_row[...] = gain_in[...][None, :]
    pack(0, pos_in[...][None, :].astype(jnp.float32))

    def norm_rows(where):
        own = xbuf[0, where, :].astype(jnp.float32)
        other = oth[where, :].astype(jnp.float32)
        total = jnp.sum(own * own, -1, keepdims=True) + jnp.sum(other * other, -1, keepdims=True)
        factor = lax.rsqrt(total * (1.0 / (2 * half)) + 1e-06)
        factor_ref[where, :] = jnp.broadcast_to(factor, (strip, HEAD_DIM))
        xbuf[0, where, :] = (own * factor * gain_row[:, features(c)]).astype(jnp.bfloat16)

    def norm_quarter(j):
        if j == 0:
            own_tokens.wait()
        if j == 1:
            rest = oth.at[pl.ds(0, rows - quarter)]
            pltpu.make_async_copy(rest, rest, tok_sem.at[2]).wait()
        each(0, subs, lambda i: norm_rows(band(lax.rem(z + j, line), i, strip)))

    def norm_far(q):
        def one(i):
            where = band(q, i, strip)
            raw = xbuf[1, where, :].astype(jnp.float32)
            normed = raw * factor_ref[where, 0:1] * gain_row[:, features(c)]
            near[pl.ds(pl.multiple_of(i * strip, strip), strip), :] = normed.astype(jnp.bfloat16)

        each(0, subs, one)

    def product(rows_in, s):
        return jnp.dot(rows_in, wbuf[s], preferred_element_type=jnp.float32)

    def tile(t):
        return pl.ds(pl.multiple_of(t * tall, tall), tall)

    loaded = set()

    def load(s):
        if s not in loaded:
            loaded.add(s)
            pltpu.make_async_copy(wbuf.at[s], wbuf.at[s], w_sem.at[s]).wait()

    def own_product(i):
        load(i)

        def one(t):
            psend[0, i, tile(t), :] = product(xbuf[0, tile(t), :], i).astype(jnp.bfloat16)

        each(0, tiles, one)
        for t in range(tiles):
            p_copy(i, t).start()

    def own_local(i):
        load(mine + i)

        def one(t):
            acc[0, i, tile(t), :] = product(xbuf[0, tile(t), :], mine + i)

        each(0, tiles, one)

    def far_product(i, s):
        load(i)
        where = band(stage_quarter(s))
        psend[1, i, where, :] = product(near[...], i).astype(jnp.bfloat16)

    def far_local(i, s):
        load(mine + i)
        where = band(stage_quarter(s))
        acc[1, i, where, :] = product(near[...], mine + i)

    def angles(slot):
        where = pl.ds(slot * rows, rows)
        lanes = unpack(slot, 0)
        kpos_ref[:, where] = jnp.broadcast_to(lanes, (8, rows))
        qpos = jnp.transpose(jnp.broadcast_to(lanes, (HEAD_DIM, rows)), (1, 0))
        qpos_ref[where, :] = qpos
        angle = qpos * freq_in[...]
        lane = lax.broadcasted_iota(jnp.int32, angle.shape, 1)
        sine = jnp.sin(angle)
        cos_ref[where, :] = jnp.cos(angle)
        sin_ref[where, :] = jnp.where(lane < HEAD_DIM // 2, -sine, sine)

    def finish(i, slot):
        def one(t):
            where = tile(t)
            at = pl.ds(pl.multiple_of(slot * rows + t * tall, tall), tall)
            field = acc[slot, i, where, :] + precv[slot, i, where, :].astype(jnp.float32)
            cosine, sine = cos_ref[at, :], sin_ref[at, :]

            def rope(x):
                return x * cosine + pltpu.roll(x, HEAD_DIM // 2, 1) * sine

            kbuf[i, at, :] = rope(field[:, :HEAD_DIM]).astype(jnp.bfloat16)
            vbuf[i, at, :HEAD_DIM] = field[:, HEAD_DIM : 2 * HEAD_DIM].astype(jnp.bfloat16)
            for h in range(2):
                one = field[:, (2 + h) * HEAD_DIM : (3 + h) * HEAD_DIM]
                qbuf[i, at, h * HEAD_DIM : (h + 1) * HEAD_DIM] = (rope(one) * query_scale).astype(jnp.bfloat16)

        each(0, tiles, one)

    def attend(i, slot, t, store):
        at = pl.ds(pl.multiple_of(slot * rows + t * tall, tall), tall)
        for h in range(2):
            both = None
            for part in range(2):
                span = pl.ds(part * rows, rows)
                scores = lax.dot_general(
                    qbuf[i, at, h * HEAD_DIM : (h + 1) * HEAD_DIM], kbuf[i, span, :],
                    (((1,), (1,)), ((), ())), preferred_element_type=jnp.float32,
                )
                allowed = kpos_ref[0:1, span] <= qpos_ref[at, 0:1]
                capped = jnp.tanh(scores * (1.0 / 50.0)) * (50.0 * math.log2(math.e))
                weights = jnp.where(allowed, jnp.exp2(capped), 0.0).astype(jnp.bfloat16)
                more = jnp.dot(weights, vbuf[i, span, :], preferred_element_type=jnp.float32)
                both = more if both is None else both + more
            done = (both[:, :HEAD_DIM] / both[:, HEAD_DIM:]).astype(jnp.bfloat16)
            store(h, done)

    def attend_far(i):
        for t in range(tiles):
            def store(h, done, t=t):
                obuf[i, t * tall : (t + 1) * tall, h * HEAD_DIM : (h + 1) * HEAD_DIM] = done

            attend(i, 1, t, store)
            o_copy(i, t, c).start()

    def attend_own(i):
        def one(t):
            def store(h, done):
                out_ref[tile(t), pl.ds(pl.multiple_of((c * mine + i) * BLOCK + h * HEAD_DIM, HEAD_DIM), HEAD_DIM)] = done

            attend(i, 0, t, store)

        each(0, tiles, one)

    def pass_on(r):
        if r < subs:
            x_copy(r).wait_recv()

            @pl.when(z < last)
            def _():
                up_copy(r, 0).start()

            @pl.when(z > 0)
            def _():
                dn_copy(r, 0).start()

        e = r - 1
        if 0 <= e < last * subs:
            @pl.when(z >= 1 + e // subs)
            def _():
                up_copy(e, 1).wait_recv()
                if e + subs < last * subs:
                    @pl.when(z < last)
                    def _():
                        up_copy(e + subs, 0).start()

            @pl.when(z + 1 + e // subs <= last)
            def _():
                dn_copy(e, 1).wait_recv()
                if e + subs < last * subs:
                    @pl.when(z > 0)
                    def _():
                        dn_copy(e + subs, 0).start()

    def stage(s):
        norm_far(stage_quarter(s))
        far_product(0, s)
        r_copy(0, s).start()
        for i in range(1, mine):
            far_product(i, s)
            early = line - HELD
            for done in range(early) if s == last - 1 else range(early, line) if s == last else ():
                r_copy(i, done).start()
        for i in range(mine):
            far_local(i, s)

    def far_side():
        side_copy().wait_recv()
        lanes = jnp.broadcast_to(unpack(1, pieces), (HEAD_DIM, rows))
        factor_ref[...] = jnp.transpose(lanes, (1, 0))

    rounds = 1 + last * subs
    work = {r: [] for r in range(rounds)}
    stage_at = [subs - 1] + [s * subs for s in range(1, line)]
    for s in range(line - 1):
        work[stage_at[s]].append(functools.partial(stage, s))
    work[stage_at[0]].insert(0, far_side)
    fill = [functools.partial(own_product, i) for i in range(mine)]
    fill += [functools.partial(angles, 0)]
    fill += [functools.partial(own_local, i) for i in range(mine)]
    fill += [functools.partial(angles, 1)]

    for j in range(line):
        norm_quarter(j)
        if j == WAIT_QUARTERS - 1:
            @pl.when(jnp.logical_not(first))
            def _():
                for i in range(subs):
                    x_copy(i).start()

    pack(pieces, jnp.transpose(factor_ref[...], (1, 0))[0:1, :])
    side_copy().start()
    for r in range(rounds):
        pass_on(r)
        if work[r]:
            for task in work[r]:
                task()
        elif fill:
            fill.pop(0)()
    for task in fill:
        task()

    stage(last)
    for i in range(mine):
        arrived(precv.at[1, i], p_recv.at[i])
        finish(i, 1)
    for i in range(mine):
        arrived(precv.at[0, i], r_recv.at[i])
        finish(i, 0)
        attend_far(i)
        attend_own(i)
    arrived(obuf, o_recv)

    side_copy().wait_send()
    sent(xbuf.at[1, band(z)], x_send)
    for k in range(last):
        @pl.when((z < last) & (z >= k))
        def _(k=k):
            sent(xbuf.at[1, band(z - k)], up_send.at[k])

        @pl.when((z > 0) & (z + k <= last))
        def _(k=k):
            sent(xbuf.at[1, band(z + k)], dn_send.at[k])

    sent(psend, p_send)
    sent(obuf, o_send)


def rope_freq():
    half = HEAD_DIM // 2
    freq = 10000.0 ** (-np.arange(half) * 2.0 / HEAD_DIM)
    return np.concatenate([freq, freq])[None, :].astype(np.float32)


def on_pair(line, tokens, token_pos, norm_gain, query_weight, key_weight, value_weight):
    rows, width = tokens.shape
    depth, q_cols = query_weight.shape
    heads = key_weight.shape[1] // HEAD_DIM
    mine = heads // 2
    subs = max(rows // line // 32, 1)
    dma = pltpu.SemaphoreType.DMA
    vmem = pl.BlockSpec(memory_space=pltpu.VMEM)
    hbm = pl.BlockSpec(memory_space=pltpu.HBM)
    ins = (token_pos, jnp.asarray(rope_freq()), norm_gain, tokens, query_weight, key_weight, value_weight)
    held = [pltpu.with_memory_space_constraint(x, pltpu.HBM) for x in ins]
    bf16, f32 = jnp.bfloat16, jnp.float32
    along = max((line - 1) * subs, 1)
    attended = pl.pallas_call(
        functools.partial(pair_kernel, line),
        out_shape=pltpu.VMEM((rows, q_cols), bf16),
        in_specs=[hbm] * 7,
        out_specs=vmem,
        scratch_shapes=[
            pltpu.VMEM((2, rows, depth), bf16),
            pltpu.VMEM((rows, depth), bf16),
            pltpu.VMEM((rows // line, depth), bf16),
            pltpu.VMEM((heads, depth, 2 * BLOCK), bf16),
            pltpu.VMEM((2, mine, rows, 2 * BLOCK), bf16),
            pltpu.VMEM((2, mine, rows, 2 * BLOCK), bf16),
            pltpu.VMEM((2, mine, rows, 2 * BLOCK), f32),
            pltpu.VMEM((mine, 2 * rows, HEAD_DIM), bf16),
            pltpu.VMEM((mine, 2 * rows, BLOCK), bf16),
            pltpu.VMEM((mine, 2 * rows, BLOCK), bf16),
            pltpu.VMEM((mine, rows, BLOCK), bf16),
            pltpu.VMEM((2 * rows, HEAD_DIM), f32),
            pltpu.VMEM((2 * rows, HEAD_DIM), f32),
            pltpu.VMEM((2 * rows, HEAD_DIM), f32),
            pltpu.VMEM((rows, HEAD_DIM), f32),
            pltpu.VMEM((8, 2 * rows), f32),
            pltpu.VMEM((2, 2 * rows // HEAD_DIM, HEAD_DIM), f32),
            pltpu.VMEM((rows,), jnp.int32),
            pltpu.VMEM((1, HEAD_DIM), f32),
            pltpu.VMEM((width,), f32),
            pltpu.VMEM((1, width), f32),
            dma((3,)),
            dma((heads,)),
            dma((3,)),
            dma(()),
            dma(()),
            dma(()),
            dma((subs,)),
            dma((line - 1,)),
            dma((line - 1,)),
            dma((along,)),
            dma(()),
            dma((mine,)),
            dma((mine,)),
            dma(()),
            dma(()),
        ],
        compiler_params=pltpu.CompilerParams(
            collective_id=0, has_side_effects=True, vmem_limit_bytes=44 * 1024 * 1024
        ),
    )(*held)
    return attended


def solution(mesh):
    in_specs = (
        P(("grp", "ctx"), None),
        P(("grp", "ctx")),
        P(),
        P("ctx", "tp"),
        P("ctx", "tp"),
        P("ctx", "tp"),
    )
    out_specs = P(("grp", "ctx"), "tp")
    ctx, grp, line = (mesh.shape[name] for name in ("ctx", "grp", "tp"))

    def local(tokens, token_pos, norm_gain, query_weight, key_weight, value_weight):
        rows, width = tokens.shape
        depth, kv_cols = key_weight.shape
        heads = kv_cols // HEAD_DIM
        paired = ctx == 2 and width == 2 * depth and heads % 2 == 0
        paired = paired and line > 1 and rows % (line * 32) == 0 and rows % HEAD_DIM == 0
        plan = functools.partial(on_pair, line) if paired else functools.partial(on_device, ctx, grp)
        return plan(tokens, token_pos, norm_gain, query_weight, key_weight, value_weight)

    return jax.shard_map(
        local, mesh=mesh, in_specs=in_specs, out_specs=out_specs, check_vma=False,
    )
```
